256 devices in a mesh: groups: 4 (over y, x), seq: 32 (over z), batch: 2 (over core).
Axes of the slice: x: 2, y: 2, z: 32, core: 2. Of those that a mesh axis runs over, the one named last changes fastest.
The devices are a block of a 4x8x32 slice.
Arguments:
- prompt_cache: bfloat16 [32, 1024, 8, 256], P(('groups', 'batch'), 'seq'), parts along dimension 0, may hold values from -6 to 6
- prompt_states: float32 [32, 32, 16, 16384], P(('groups', 'batch'), 'seq'), parts along dimension 0, may hold values from -6 to 6
- block_steps: float32 [32, 32, 16384], P(('groups', 'batch'), 'seq'), parts along dimension 0, may hold values from 0.005 to 0.1
- prompt_lengths: int32 [32], P('groups'), parts along dimension 0, may hold values from 170 to 1023
- target_slots: int32 [32], P('groups'), parts along dimension 0, may hold values from 0 to 15, as said below
- cache_lengths: int32 [64], P(('groups', 'batch')), parts along dimension 0, may hold values from 170 to 1023
- resident_cache: bfloat16 [64, 32, 32, 8, 256], P(('groups', 'batch'), None, 'seq'), parts along dimension 0, may hold values from -6 to 6
- token_cache: bfloat16 [64, 8, 256], P(('groups', 'batch')), parts along dimension 0, may hold values from -6 to 6
- queries: bfloat16 [64, 64, 128], P(('groups', 'batch')), parts along dimension 0, may hold values from -6 to 6
- resident_states: float32 [64, 16, 16384], P(('groups', 'batch'), None, 'seq'), parts along dimension 0, may hold values from -6 to 6
- decay_rates: float32 [16, 16384], replicated, may hold values from 0.05 to 10
- step_sizes: float32 [64, 16384], P(('groups', 'batch'), 'seq'), parts along dimension 0, may hold values from 0.01 to 1
- inner_input: bfloat16 [64, 16384], P(('groups', 'batch'), 'seq'), parts along dimension 0, may hold values from -6 to 6
- inner_gate: bfloat16 [64, 16384], P(('groups', 'batch'), 'seq'), parts along dimension 0, may hold values from -6 to 6
- state_input: float32 [64, 16], P(('groups', 'batch')), parts along dimension 0, may hold values from -6 to 6
- state_readout: float32 [64, 16], P(('groups', 'batch')), parts along dimension 0, may hold values from -6 to 6
- skip_gain: float32 [16384], P('seq'), may hold values from 0.5 to 1.5
Outputs:
- merged_cache: bfloat16 [64, 32, 32, 8, 256], P(('groups', 'batch'), None, 'seq'), parts along dimension 0
- attention: bfloat16 [64, 64, 128], P(('groups', 'batch'), 'seq'), parts along dimension 0
- next_states: float32 [64, 16, 16384], P(('groups', 'batch'), None, 'seq'), parts along dimension 0
- mamba_output: bfloat16 [64, 16384], P(('groups', 'batch'), 'seq'), parts along dimension 0
The draws below stay inside these ranges and needn't reach their ends.
There are 4 independent parts, one for each index of `groups`. The reference program is written for one: setup_inputs(seed, part) draws one part's arguments, and reference() takes and returns one part's arrays. A program takes and returns all parts, laid end to end along the dimension named above; an argument that names none is the same for every part. Nothing has to cross between parts.
Inputs may be any that keep to these rules, and one draw needn't show every extreme that they name: `target_slots`: 8 distinct slots.
All inputs are finite; a program needn't handle non-finite values.
Results may differ from the reference program's by a relative error of at most 0.0019.
Values may be sent and summed in bfloat16 or wider, within the bound.
A program may use at most 320 MiB of HBM per device.

```python
import math
import jax
import jax.numpy as jnp
from jax import lax

HEADS = 64
KV_HEADS = 8
HEAD_DIM = 128
INNER = 16384
STATE = 16
PROMPTS = 8
BLOCK_LEN = 32
SLOTS_DEV = 8
PROMPT_MAX = 1024
SLOTS = 16
N_SEQ = 32
N_BATCH = 2


def draw_target_slots(key, part):
    shuffled = jax.random.permutation(key, SLOTS)
    return shuffled[:PROMPTS].astype(jnp.int32)


def sign_direction(key):
    return jax.random.rademacher(jax.random.fold_in(key, 7101), (KV_HEADS, HEAD_DIM), dtype=jnp.float32)


def key_amplitudes():
    return jnp.array([4.8, 4.76, 4.72], jnp.float32)


def keyed_cache(key, row_count, salt_value, level_set):
    kv_width = 2 * HEAD_DIM
    noise_key, spot_key, fine_key = jax.random.split(jax.random.fold_in(key, salt_value), 3)
    base_draw = jnp.clip(jax.random.normal(noise_key, (row_count, PROMPT_MAX, KV_HEADS, kv_width), jnp.float32), -6.0, 6.0)
    reach_len = max(PROMPT_MAX // 6, 3)

    def pick_spots(row_index):
        return jax.random.permutation(jax.random.fold_in(spot_key, row_index), reach_len)[:3].astype(jnp.int32)
    spot_rows = jax.vmap(pick_spots)(jnp.arange(row_count, dtype=jnp.int32))
    position = jnp.arange(PROMPT_MAX, dtype=jnp.int32)
    hit_table = (position[None, None, :] == spot_rows[:, :, None]).astype(jnp.float32)
    amplitude = jnp.einsum('rkt,k->rt', hit_table, level_set)
    chosen = jnp.sum(hit_table, axis=1)
    direction = sign_direction(key)
    fine_noise = 0.02 * jnp.clip(jax.random.normal(fine_key, (row_count, PROMPT_MAX, KV_HEADS, HEAD_DIM), jnp.float32), -3.0, 3.0)
    aligned = amplitude[:, :, None, None] * direction[None, None] + fine_noise
    new_keys = jnp.where(chosen[:, :, None, None] > 0.5, aligned, base_draw[..., :HEAD_DIM])
    return jnp.concatenate([new_keys, base_draw[..., HEAD_DIM:]], axis=3)


def draw_prompt_cache(key, part):
    level_set = key_amplitudes()
    return keyed_cache(key, PROMPTS, 11, level_set).astype(jnp.bfloat16)


def draw_resident_cache(key, part):
    level_set = key_amplitudes()
    filled = keyed_cache(key, SLOTS, 13, level_set)
    return filled.reshape(SLOTS, BLOCK_LEN, -1, KV_HEADS, 2 * HEAD_DIM).astype(jnp.bfloat16)


def draw_queries(key, part):
    group_size = HEADS // KV_HEADS
    direction = sign_direction(key)
    head_dirs = jnp.repeat(direction, group_size, axis=0)
    mask_key, level_key, noise_key, fine_key = jax.random.split(jax.random.fold_in(key, 17), 4)
    drawn = jnp.clip(jax.random.normal(noise_key, (SLOTS, HEADS, HEAD_DIM), jnp.float32), -6.0, 6.0)
    picked = jax.random.bernoulli(mask_key, 0.25, (SLOTS, HEADS))
    strength = jax.random.uniform(level_key, (SLOTS, HEADS), jnp.float32, 2.2, 5.5)
    fine_noise = 0.1 * jnp.clip(jax.random.normal(fine_key, (SLOTS, HEADS, HEAD_DIM), jnp.float32), -3.0, 3.0)
    aligned = jnp.clip(strength[..., None] * head_dirs[None] + fine_noise, -6.0, 6.0)
    return jnp.where(picked[..., None], aligned, drawn).astype(jnp.bfloat16)


def set_ends(result, key, least, top_value):
    place = [jax.random.randint(jax.random.fold_in(key, axis), (), 0, length) for axis, length in enumerate(result.shape)]
    longest = result.shape.index(max(result.shape))
    neighbour = place[:longest] + [(place[longest] + 1) % result.shape[longest]] + place[longest + 1:]
    return result.at[tuple(place)].set(least).at[tuple(neighbour)].set(top_value)


def strengthened(drawn, own_key, source, target, parts, factor):
    def block_of(axis_at):
        return (jnp.arange(drawn.shape[axis_at]) // (drawn.shape[axis_at] // parts)).reshape((-1,) + (1,) * (drawn.ndim - 1 - axis_at))

    near = jax.random.permutation(own_key, parts)[block_of(target)]
    other_side = (block_of(target) + parts // 2) % parts
    return jnp.where((block_of(source) == near) | (block_of(source) == other_side), factor * drawn, drawn)


def block_scale(stream_key, extent, pieces, least, top_value):
    def one(dim, parts):
        draws = jax.random.uniform(jax.random.fold_in(jax.random.fold_in(stream_key, 6), dim), (parts,), jnp.float32, least / len(pieces), top_value / len(pieces))
        return jnp.repeat(jnp.exp(draws), extent[dim] // parts).reshape((-1,) + (1,) * (len(extent) - dim - 1))

    level = one(*pieces[0])
    for cut in pieces[1:]:
        level = level * one(*cut)
    return level


def gaussian(key, extent, width, reach, shards=(), held_as=jnp.bfloat16):
    drawn = jax.random.normal(key, extent, jnp.float32) * width
    if len(shards) > 0:
        drawn = block_scale(key, extent, shards, -0.22, 0.18) * drawn
    return jnp.clip(drawn, min=-reach, max=reach).astype(held_as)


def heavy_noise(own_key, extent, spread, bound, cuts, heavy, held_as=jnp.bfloat16):
    values = spread * jax.random.normal(own_key, extent, jnp.float32)
    if cuts:
        values = values * block_scale(own_key, extent, cuts, -0.22, 0.18)
    return jnp.clip(strengthened(values, jax.random.fold_in(own_key, 3), *heavy), -bound, bound).astype(held_as)


def setup_inputs(seed: int = 0, part: int = 0) -> dict:
    key_list = jax.random.split(jax.random.key(seed), 18)
    part_keys = jax.random.split(jax.random.fold_in(key_list[17], part), 18)
    prompt_cache = draw_prompt_cache(jax.random.fold_in(jax.random.fold_in(key_list[17], part), 71), part)
    prompt_states = heavy_noise(part_keys[1], (PROMPTS, N_SEQ, STATE, INNER), 1.0, 6.0, ((0, 2), (1, 32)), (1, 3, 32, 2.75), jnp.float32)
    block_steps = jnp.clip(jnp.exp(math.log(0.1) - 2.9957323 * jax.random.uniform(part_keys[2], (PROMPTS, N_SEQ, INNER), jnp.float32) ** block_scale(part_keys[2], (PROMPTS, N_SEQ, INNER), ((0, 2), (1, 32)), -0.2, 0.2)), 0.005, 0.1)
    prompt_lengths = set_ends(jax.random.randint(part_keys[3], (PROMPTS,), PROMPT_MAX // 6, PROMPT_MAX), jax.random.fold_in(part_keys[3], 1), PROMPT_MAX // 6, PROMPT_MAX - 1).astype(jnp.int32)
    target_slots = draw_target_slots(jax.random.fold_in(jax.random.fold_in(key_list[17], part), 71), part)
    cache_lengths = set_ends(jax.random.randint(part_keys[5], (SLOTS,), PROMPT_MAX // 6, PROMPT_MAX), jax.random.fold_in(part_keys[5], 1), PROMPT_MAX // 6, PROMPT_MAX - 1).astype(jnp.int32)
    resident_cache = draw_resident_cache(jax.random.fold_in(jax.random.fold_in(key_list[17], part), 71), part)
    token_cache = gaussian(part_keys[7], (SLOTS, KV_HEADS, 2 * HEAD_DIM), 1.0, 6.0, ((0, 2),))
    queries = draw_queries(jax.random.fold_in(jax.random.fold_in(key_list[17], part), 71), part)
    resident_states = gaussian(part_keys[9], (SLOTS, STATE, INNER), 1.0, 6.0, ((0, 2), (2, 32)), jnp.float32)
    decay_rates = jnp.clip(jnp.exp(jax.random.uniform(key_list[10], (STATE, INNER), jnp.float32, math.log(0.05), math.log(10.0))), 0.05, 10.0)
    step_sizes = jnp.clip(jnp.exp(math.log(1.0) - 4.6051702 * jax.random.uniform(part_keys[11], (SLOTS, INNER), jnp.float32) ** block_scale(part_keys[11], (SLOTS, INNER), ((0, 2), (1, 32)), -0.2, 0.2)), 0.01, 1.0)
    inner_input = gaussian(part_keys[12], (SLOTS, INNER), 1.0, 6.0, ((0, 2), (1, 32)))
    inner_gate = gaussian(part_keys[13], (SLOTS, INNER), 1.0, 6.0, ((0, 2), (1, 32)))
    state_input = gaussian(part_keys[14], (SLOTS, STATE), 1.0, 6.0, ((0, 2),), jnp.float32)
    state_readout = gaussian(part_keys[15], (SLOTS, STATE), 1.0, 6.0, ((0, 2),), jnp.float32)
    skip_gain = jnp.clip(0.5 + 1.0 * jax.random.uniform(key_list[16], (INNER,), jnp.float32) ** block_scale(key_list[16], (INNER,), ((0, 32),), -0.2, 0.2), 0.5, 1.5)
    return {"prompt_cache": prompt_cache, "prompt_states": prompt_states, "block_steps": block_steps, "prompt_lengths": prompt_lengths, "target_slots": target_slots, "cache_lengths": cache_lengths, "resident_cache": resident_cache, "token_cache": token_cache, "queries": queries, "resident_states": resident_states, "decay_rates": decay_rates, "step_sizes": step_sizes, "inner_input": inner_input, "inner_gate": inner_gate, "state_input": state_input, "state_readout": state_readout, "skip_gain": skip_gain}


def reference(prompt_cache, prompt_states, block_steps, prompt_lengths, target_slots, cache_lengths, resident_cache, token_cache, queries, resident_states, decay_rates, step_sizes, inner_input, inner_gate, state_input, state_readout, skip_gain):
    prompt_max = BLOCK_LEN * N_SEQ
    slot_count = SLOTS_DEV * N_BATCH
    kv_width = 2 * HEAD_DIM
    slot_ids = jnp.arange(slot_count, dtype=jnp.int32)
    matches = target_slots[None, :] == slot_ids[:, None]
    fresh = jnp.any(matches, axis=1)
    chosen_len = lax.optimization_barrier(jnp.sum(jnp.where(matches, prompt_lengths[None, :], 0), axis=1)).astype(jnp.int32)
    lengths = jnp.where(fresh, chosen_len, cache_lengths).astype(jnp.int32)
    picked = jnp.dot(matches.astype(jnp.bfloat16), prompt_cache.reshape(PROMPTS, -1), preferred_element_type=jnp.float32)
    picked = picked.astype(jnp.bfloat16).reshape(slot_count, prompt_max, KV_HEADS, kv_width)
    resident = resident_cache.reshape(slot_count, prompt_max, KV_HEADS, kv_width)
    position = jnp.arange(prompt_max, dtype=jnp.int32)
    merged = jnp.where(fresh[:, None, None, None], picked, resident)
    merged = jnp.where((position[None, :] < lengths[:, None])[:, :, None, None], merged, jnp.zeros((), jnp.bfloat16))
    merged = jnp.where((position[None, :] == lengths[:, None])[:, :, None, None], token_cache[:, None], merged)
    merged_cache = merged.reshape(slot_count, BLOCK_LEN, N_SEQ, KV_HEADS, kv_width)
    group = HEADS // KV_HEADS
    grouped = queries.reshape(slot_count, KV_HEADS, group, HEAD_DIM).astype(jnp.float32)
    scores = jnp.einsum('rgqd,rtgd->rgqt', grouped, merged[..., :HEAD_DIM].astype(jnp.float32)) * (1.0 / math.sqrt(HEAD_DIM))
    seen = (position[None, :] <= lengths[:, None])[:, None, None, :]
    masked = jnp.where(seen, scores, -1e+30)
    masked = masked.reshape(slot_count, KV_HEADS, group, BLOCK_LEN, N_SEQ)
    seen_cls = jnp.broadcast_to(seen, scores.shape).reshape(slot_count, KV_HEADS, group, BLOCK_LEN, N_SEQ)
    class_top = lax.optimization_barrier(jnp.max(masked, axis=3))
    weights = jnp.where(seen_cls, jnp.exp(masked - class_top[:, :, :, None, :]), 0.0)
    class_total = lax.optimization_barrier(jnp.sum(weights, axis=3))
    values = merged_cache[..., HEAD_DIM:].astype(jnp.float32)
    class_sum = jnp.einsum('rgqij,rijgd->rgqjd', weights.astype(jnp.bfloat16).astype(jnp.float32), values)
    overall = lax.optimization_barrier(jnp.max(class_top, axis=3))
    factor = jnp.exp(class_top - overall[..., None])
    total = lax.optimization_barrier(jnp.sum(class_total * factor, axis=3))
    summed = lax.optimization_barrier(jnp.sum(class_sum * factor[..., None], axis=3))
    attention = (summed / total[..., None]).reshape(slot_count, HEADS, HEAD_DIM).astype(jnp.bfloat16)
    starts = jnp.arange(N_SEQ, dtype=jnp.int32) * BLOCK_LEN
    usable = (starts[None, :] < prompt_lengths[:, None]).astype(jnp.float32)
    step_terms = block_steps * usable[:, :, None]
    later = lax.optimization_barrier(jnp.sum(step_terms, axis=1, keepdims=True)) - jnp.cumsum(step_terms, axis=1)

    def fold_prompt(packed):
        states, behind, weight = packed
        return lax.optimization_barrier(jnp.sum(weight[:, None, None] * jnp.exp(-decay_rates[None] * behind[:, None, :]) * states, axis=0))
    handed = lax.map(fold_prompt, (prompt_states, later, usable))
    chosen_state = jnp.einsum('rp,pnc->rnc', matches.astype(jnp.float32), handed, precision=lax.Precision.HIGHEST)
    start = jnp.where(fresh[:, None, None], chosen_state, resident_states)
    inner = inner_input.astype(jnp.float32)
    next_states = jnp.exp(-decay_rates[None] * step_sizes[:, None, :]) * start + (step_sizes * inner)[:, None, :] * state_input[:, :, None]
    readout = lax.optimization_barrier(jnp.sum(state_readout[:, :, None] * next_states, axis=1)) + skip_gain[None, :] * inner
    mamba_output = (readout * jax.nn.silu(inner_gate.astype(jnp.float32))).astype(jnp.bfloat16)
    return (merged_cache, attention, next_states, mamba_output)
```

```python
import functools
import math

import jax
import jax.numpy as jnp
from jax import lax
from jax.experimental import pallas as pl
from jax.experimental.pallas import tpu as pltpu
from jax.sharding import PartitionSpec as P

MESH = pl.DeviceIdType.MESH
STEPS_BEFORE_ATTENTION = 5


def kernel(
    n,
    early,
    plen_ref,
    target_ref,
    clen_ref,
    cache_ref,
    steps_ref,
    states_hbm,
    rates,
    resident,
    token_ref,
    query_ref,
    res_state_ref,
    step_size_ref,
    inner_ref,
    gate_ref,
    sin_ref,
    sout_ref,
    skip_ref,
    merged,
    att_ref,
    next_ref,
    mamba_ref,
    states,
    msteps,
    arrived,
    t_up,
    t_dn,
    h_up,
    h_dn,
    r_up,
    r_dn,
    s_up,
    s_dn,
    part_sum,
    part_ml,
    handed,
    load_sem,
    cache_send,
    cache_recv,
    pair_send,
    pair_recv,
    t_send,
    t_recv,
    h_send,
    h_recv,
    r_send,
    r_recv,
    s_send,
    s_recv,
):
    h = n // 2
    me = lax.axis_index("seq")
    core = lax.axis_index("batch")
    up = lax.rem(me + 1, n)
    down = lax.rem(me + n - 1, n)
    prompts, block_len, kv_heads, kv_width = cache_ref.shape
    state = states.shape[1]
    share = handed.shape[3]
    slots, heads, head_dim = query_ref.shape
    rows = block_len * kv_heads
    own_heads = heads // n
    group = heads // kv_heads

    barrier = pltpu.get_barrier_semaphore()

    def greet(k, carry):
        pl.semaphore_signal(
            barrier, inc=1, device_id={"seq": lax.rem(me + k, n)}, device_id_type=MESH
        )
        return carry

    lax.fori_loop(1, n, greet, 0)
    pl.semaphore_signal(barrier, inc=1, device_id={"batch": 1 - core}, device_id_type=MESH)

    load = pltpu.make_async_copy(states_hbm, states, load_sem)
    load.start()

    usable = []
    for p in range(prompts):
        reached = me * block_len < plen_ref[core * prompts + p]
        usable.append(jnp.where(reached, 1.0, 0.0).astype(jnp.float32))
        msteps[p : p + 1, :] = steps_ref[p : p + 1, :] * usable[p]

    def columns(o):
        return pl.ds(pl.multiple_of(o * share, share), share)

    def remote(src, dst, send, recv, where):
        return pltpu.make_async_remote_copy(
            src_ref=src,
            dst_ref=dst,
            send_sem=send,
            recv_sem=recv,
            device_id=where,
            device_id_type=MESH,
        )

    def hop(buf, k, send, recv, to):
        return remote(buf.at[k], buf.at[k + 1], send, recv.at[k + 1], {"seq": to})

    def arrival(buf, k, send, recv, to):
        return remote(buf.at[k], buf.at[k], send, recv.at[k], {"seq": to})

    for p in range(prompts):
        arrived[p, me] = cache_ref[p, me]

    pl.semaphore_wait(barrier, n)

    def add_steps(s):
        o = lax.rem(s + n - h, n)
        mine = msteps[:, columns(o)]
        high = jnp.where(me > s, 1.0, 0.0).astype(jnp.float32)
        return high * mine, (1.0 - high) * mine

    def send_cache(k):
        to = lax.rem(me + k, n)
        remote(
            cache_ref.at[:, to], arrived.at[pl.ds(0, prompts), me], cache_send, cache_recv, {"seq": to}
        ).start()

    def first_steps(buf, s):
        above, below = add_steps(s)
        buf[0, 0:prompts, :] = above
        buf[0, prompts : 2 * prompts, :] = below

    def more_steps(buf, k, s):
        above, below = add_steps(s)
        buf[k, 0:prompts, :] += above
        buf[k, prompts : 2 * prompts, :] += below

    first_steps(t_up, lax.rem(me + h - 1, n))
    first_steps(t_dn, lax.rem(me + n - h, n))
    hop(t_up, 0, t_send.at[0], t_recv.at[0], up).start()
    hop(t_dn, 0, t_send.at[1], t_recv.at[1], down).start()
    send_cache(1)
    send_cache(n - 1)

    def step_ring(k, carry):
        arrival(t_up, k, t_send.at[0], t_recv.at[0], up).wait_recv()
        more_steps(t_up, k, lax.rem(me + h - 1 - k, n))

        @pl.when(k < h - 1)
        def _():
            hop(t_up, k, t_send.at[0], t_recv.at[0], up).start()

        arrival(t_dn, k, t_send.at[1], t_recv.at[1], down).wait_recv()
        more_steps(t_dn, k, lax.rem(me + n - h + k, n))
        hop(t_dn, k, t_send.at[1], t_recv.at[1], down).start()
        send_cache(k + 1)

        @pl.when(k < h - 1)
        def _():
            send_cache(n - 1 - k)

        return carry

    lax.fori_loop(1, h, step_ring, 0)
    arrival(t_dn, h, t_send.at[1], t_recv.at[1], down).wait_recv()
    later = t_up[h - 1, 0:prompts, :] + t_dn[h, 0:prompts, :]
    everything = (
        later + t_up[h - 1, prompts : 2 * prompts, :] + t_dn[h, prompts : 2 * prompts, :]
    )

    load.wait()

    def term(p, o, behind):
        return (
            usable[p]
            * jnp.exp(-rates[:, columns(o)] * behind)
            * states[p, :, columns(o)]
        )

    start = lax.rem(me + n - h, n)
    h_up[0, 0:prompts, :] = later
    h_up[0, prompts : 2 * prompts, :] = everything
    hop(h_up, 0, h_send.at[0], h_recv.at[0], up).start()
    h_dn[0, 0:prompts, :] = later + msteps[:, columns(start)]
    h_dn[0, prompts : 2 * prompts, :] = everything
    hop(h_dn, 0, h_send.at[1], h_recv.at[1], down).start()

    def send_sum(way, buf, k, p, to):
        remote(
            buf.at[k, p], buf.at[k + 1, p], r_send.at[way], r_recv.at[way, k + 1, p], {"seq": to}
        ).start()

    def wait_sum(way, buf, k, p, to):
        remote(
            buf.at[k, p], buf.at[k, p], r_send.at[way], r_recv.at[way, k, p], {"seq": to}
        ).wait_recv()

    for p in range(prompts):
        r_dn[0, p] = term(p, start, later[p : p + 1])
        send_sum(1, r_dn, 0, p, down)

    def header_up(k, o):
        arrival(h_up, k, h_send.at[0], h_recv.at[0], up).wait_recv()
        before = jnp.where(me == 0, h_up[k, prompts : 2 * prompts, :], h_up[k, 0:prompts, :])
        return before - msteps[:, columns(o)]

    def state_step(k, first):
        o_up = lax.rem(me + 2 * n - h - k, n)
        o_dn = lax.rem(me + n - h + k, n)
        behind_up = header_up(k, o_up)
        h_up[k, 0:prompts, :] = behind_up
        hop(h_up, k, h_send.at[0], h_recv.at[0], up).start()
        arrival(h_dn, k, h_send.at[1], h_recv.at[1], down).wait_recv()
        behind_dn = jnp.where(me == n - 1, 0.0, h_dn[k, 0:prompts, :])
        h_dn[k, 0:prompts, :] = behind_dn + msteps[:, columns(o_dn)]

        @pl.when(k < h - 1)
        def _():
            hop(h_dn, k, h_send.at[1], h_recv.at[1], down).start()

        for p in range(prompts):
            up_term = term(p, o_up, behind_up[p : p + 1])
            if first:
                r_up[k, p] = up_term
            else:
                wait_sum(0, r_up, k, p, up)
                r_up[k, p] += up_term
            send_sum(0, r_up, k, p, up)
            dn_term = term(p, o_dn, behind_dn[p : p + 1])
            wait_sum(1, r_dn, k, p, down)
            r_dn[k, p] += dn_term
            send_sum(1, r_dn, k, p, down)

    state_step(1, True)
    lax.fori_loop(2, early, lambda k, c: (state_step(k, False), c)[1], 0)

    remote(
        cache_ref.at[:, pl.ds(0, n - 1)],
        arrived.at[pl.ds(0, prompts), pl.ds(0, n - 1)],
        cache_send,
        cache_recv,
        {"seq": up},
    ).wait()
    cache_pair = remote(
        arrived.at[pl.ds(0, prompts)],
        arrived.at[pl.ds(prompts, prompts)],
        pair_send.at[0],
        pair_recv.at[0],
        {"batch": 1 - core},
    )
    cache_pair.start()
    cache_pair.wait()

    def slot_facts(r):
        slot = core * slots + r
        fresh, length, place = jnp.int32(0), clen_ref[r], jnp.int32(0)
        for q in range(2 * prompts):
            index = lax.rem(core * prompts + q, 2 * prompts)
            hit = target_ref[index] == slot
            fresh = jnp.where(hit, 1, fresh)
            length = jnp.where(hit, plen_ref[index], length)
            place = jnp.where(hit, q, place)
        return fresh == 1, length, place

    def attend(r, carry):
        fresh, length, place = slot_facts(r)
        chosen = jnp.where(
            fresh, arrived[place].astype(jnp.float32), resident[r].astype(jnp.float32)
        )
        position = lax.broadcasted_iota(jnp.int32, chosen.shape, 0) * n + me
        chosen = jnp.where(position < length, chosen, 0.0)
        token = jnp.broadcast_to(token_ref[r].astype(jnp.float32)[None], chosen.shape)
        chosen = jnp.where(position == length, token, chosen)
        merged[r] = chosen.astype(jnp.bfloat16)
        flat = chosen.reshape(rows, kv_width).astype(jnp.bfloat16)
        score = lax.dot_general(
            query_ref[r],
            flat[:, :head_dim],
            (((1,), (1,)), ((), ())),
            preferred_element_type=jnp.float32,
        ) * (1.0 / math.sqrt(head_dim))
        column = lax.broadcasted_iota(jnp.int32, score.shape, 1)
        row = lax.broadcasted_iota(jnp.int32, score.shape, 0)
        seen = (lax.rem(column, kv_heads) == lax.div(row, group)) & (
            lax.div(column, kv_heads) * n + me <= length
        )
        score = jnp.where(seen, score, -1e30)
        top = jnp.max(score, axis=1, keepdims=True)
        weight = jnp.where(seen, jnp.exp(score - top), 0.0)
        total = jnp.sum(weight, axis=1, keepdims=True)
        summed = jnp.dot(
            weight.astype(jnp.bfloat16), flat[:, head_dim:], preferred_element_type=jnp.float32
        )
        at = pl.ds(pl.multiple_of(r * heads, heads), heads)
        part_sum[at, :] = summed
        lane = lax.broadcasted_iota(jnp.int32, summed.shape, 1)
        part_ml[at, :] = jnp.where(lane < head_dim // 2, top, total)
        return carry

    lax.fori_loop(0, slots, attend, 0)

    count = own_heads * slots
    half = head_dim // 2

    def own_part(o):
        sums = [
            part_sum[pl.ds(o * own_heads + g, slots, stride=heads), :] for g in range(own_heads)
        ]
        mls = [part_ml[pl.ds(o * own_heads + g, slots, stride=heads), :] for g in range(own_heads)]
        return jnp.concatenate(sums, 0), jnp.concatenate(mls, 0)

    def joined(one, other):
        (sum_a, ml_a), (sum_b, ml_b) = one, other
        top_a, top_b = ml_a[:, 0:1], ml_b[:, 0:1]
        top = jnp.maximum(top_a, top_b)
        f_a, f_b = jnp.exp(top_a - top), jnp.exp(top_b - top)
        lane = lax.broadcasted_iota(jnp.int32, ml_a.shape, 1)
        total = ml_a * f_a + ml_b * f_b
        return sum_a * f_a + sum_b * f_b, jnp.where(lane < half, top, total)

    def read(buf, k):
        return buf[k, 0:count, :], buf[k, count : 2 * count, :]

    def put(buf, k, value):
        buf[k, 0:count, :] = value[0]
        buf[k, count : 2 * count, :] = value[1]

    put(s_up, 0, own_part(lax.rem(me + h - 1, n)))
    hop(s_up, 0, s_send.at[0], s_recv.at[0], up).start()
    put(s_dn, 0, own_part(lax.rem(me + n - h, n)))
    hop(s_dn, 0, s_send.at[1], s_recv.at[1], down).start()

    def soft_step(k):
        arrival(s_up, k, s_send.at[0], s_recv.at[0], up).wait_recv()
        put(s_up, k, joined(read(s_up, k), own_part(lax.rem(me + h - 1 - k, n))))

        @pl.when(k < h - 1)
        def _():
            hop(s_up, k, s_send.at[0], s_recv.at[0], up).start()

        arrival(s_dn, k, s_send.at[1], s_recv.at[1], down).wait_recv()
        put(s_dn, k, joined(read(s_dn, k), own_part(lax.rem(me + n - h + k, n))))
        hop(s_dn, k, s_send.at[1], s_recv.at[1], down).start()

    def both(k, carry):
        state_step(k, False)
        soft_step(k - early + 1)
        return carry

    lax.fori_loop(early, h, both, 0)

    behind = header_up(h, me)
    for p in range(prompts):
        own = term(p, me, behind[p : p + 1])
        wait_sum(0, r_up, h, p, up)
        wait_sum(1, r_dn, h, p, down)
        handed[0, p] = r_up[h, p] + r_dn[h, p] + own
    state_pair = remote(
        handed.at[0], handed.at[1], pair_send.at[1], pair_recv.at[1], {"batch": 1 - core}
    )
    state_pair.start()

    lax.fori_loop(h - early + 1, h, lambda k, c: (soft_step(k), c)[1], 0)
    state_pair.wait()

    rates_here = rates[:, columns(me)]
    inner = inner_ref[...].astype(jnp.float32)
    gate = gate_ref[...].astype(jnp.float32)
    gated = gate / (1.0 + jnp.exp(-gate))
    driven = step_size_ref[...] * inner
    skipped = skip_ref[...] * inner
    for r in range(slots):
        fresh, _, place = slot_facts(r)
        begin = jnp.where(fresh, handed[lax.div(place, prompts), lax.rem(place, prompts)], res_state_ref[r])
        following = (
            jnp.exp(-rates_here * step_size_ref[r : r + 1, :]) * begin
            + driven[r : r + 1, :] * sin_ref[:, r : r + 1]
        )
        next_ref[r] = following
        readout = jnp.sum(sout_ref[:, r : r + 1] * following, axis=0, keepdims=True)
        mamba_ref[r : r + 1, :] = (readout + skipped[r : r + 1, :]) * gated[r : r + 1, :]

    arrival(s_dn, h, s_send.at[1], s_recv.at[1], down).wait_recv()
    sums, mls = joined(read(s_up, h - 1), read(s_dn, h))
    att_ref[...] = sums / mls[:, half : half + 1]

    def sent(buf, first, last, send, recv, to):
        part = buf.at[pl.ds(first, last - first)]
        remote(part, part, send, recv, {"seq": to}).wait_send()

    sent(t_up, 0, h - 1, t_send.at[0], t_recv.at[0, 0], up)
    sent(t_dn, 0, h, t_send.at[1], t_recv.at[1, 0], down)
    sent(h_up, 0, h, h_send.at[0], h_recv.at[0, 0], up)
    sent(h_dn, 0, h - 1, h_send.at[1], h_recv.at[1, 0], down)
    sent(r_up, 1, h, r_send.at[0], r_recv.at[0, 0, 0], up)
    sent(r_dn, 0, h, r_send.at[1], r_recv.at[1, 0, 0], down)
    sent(s_up, 0, h - 1, s_send.at[0], s_recv.at[0, 0], up)
    sent(s_dn, 0, h, s_send.at[1], s_recv.at[1, 0], down)


def local(
    n,
    prompt_cache,
    prompt_states,
    block_steps,
    prompt_lengths,
    target_slots,
    cache_lengths,
    resident_cache,
    token_cache,
    queries,
    resident_states,
    decay_rates,
    step_sizes,
    inner_input,
    inner_gate,
    state_input,
    state_readout,
    skip_gain,
):
    prompts, block_len, kv_heads, kv_width = prompt_cache.shape
    slots, heads, head_dim = queries.shape
    state, channels = decay_rates.shape
    share = channels // n
    h = n // 2
    own_heads = heads // n
    count = own_heads * slots
    f32, bf16 = jnp.float32, jnp.bfloat16
    smem = pl.BlockSpec(memory_space=pltpu.SMEM)
    vmem = pl.BlockSpec(memory_space=pltpu.VMEM)
    hbm = pl.BlockSpec(memory_space=pltpu.HBM)
    dma, vm = pltpu.SemaphoreType.DMA, pltpu.VMEM
    merged, attention, next_states, mamba_output = pl.pallas_call(
        functools.partial(kernel, n, min(STEPS_BEFORE_ATTENTION, h)),
        out_shape=(
            jax.ShapeDtypeStruct((slots, block_len, kv_heads, kv_width), bf16),
            jax.ShapeDtypeStruct((count, head_dim), f32),
            jax.ShapeDtypeStruct((slots, state, share), f32),
            jax.ShapeDtypeStruct((slots, share), f32),
        ),
        in_specs=[smem] * 3 + [vmem] * 2 + [hbm] + [vmem] * 11,
        out_specs=(vmem, vmem, vmem, vmem),
        scratch_shapes=[
            vm((prompts, state, channels), f32),
            vm((prompts, channels), f32),
            vm((2 * prompts, block_len, kv_heads, kv_width), bf16),
            vm((h + 1, 2 * prompts, share), f32),
            vm((h + 1, 2 * prompts, share), f32),
            vm((h + 1, 2 * prompts, share), f32),
            vm((h + 1, 2 * prompts, share), f32),
            vm((h + 1, prompts, state, share), f32),
            vm((h + 1, prompts, state, share), f32),
            vm((h + 1, 2 * count, head_dim), f32),
            vm((h + 1, 2 * count, head_dim), f32),
            vm((slots * heads, head_dim), f32),
            vm((slots * heads, head_dim), f32),
            vm((2, prompts, state, share), f32),
            dma,
            dma,
            dma,
            dma((2,)),
            dma((2,)),
            dma((2,)),
            dma((2, h + 1)),
            dma((2,)),
            dma((2, h + 1)),
            dma((2,)),
            dma((2, h + 1, prompts)),
            dma((2,)),
            dma((2, h + 1)),
        ],
        compiler_params=pltpu.CompilerParams(
            collective_id=0, has_side_effects=True, vmem_limit_bytes=48 * 1024 * 1024
        ),
    )(
        prompt_lengths,
        target_slots,
        cache_lengths,
        prompt_cache,
        block_steps[:, 0],
        prompt_states[:, 0],
        decay_rates,
        resident_cache[:, :, 0],
        token_cache,
        queries,
        resident_states,
        step_sizes,
        inner_input,
        inner_gate,
        state_input.T,
        state_readout.T,
        skip_gain[None],
    )
    attention = attention.reshape(own_heads, slots, head_dim).transpose(1, 0, 2).astype(bf16)
    return merged[:, :, None], attention, next_states, mamba_output.astype(bf16)


def solution(mesh):
    n = mesh.shape["seq"]
    rows = ("groups", "batch")
    return jax.shard_map(
        functools.partial(local, n),
        mesh=mesh,
        in_specs=(
            P(rows, "seq", None, None),
            P(rows, "seq", None, None),
            P(rows, "seq", None),
            P("groups"),
            P("groups"),
            P(rows),
            P(rows, None, "seq", None, None),
            P(rows, None, None),
            P(rows, None, None),
            P(rows, None, "seq"),
            P(),
            P(rows, "seq"),
            P(rows, "seq"),
            P(rows, "seq"),
            P(rows, None),
            P(rows, None),
            P("seq"),
        ),
        out_specs=(
            P(rows, None, "seq", None, None),
            P(rows, "seq", None),
            P(rows, None, "seq"),
            P(rows, "seq"),
        ),
        check_vma=False,
    )
```

```python
import functools
import math

import jax
import jax.numpy as jnp
from jax import lax
from jax.experimental import pallas as pl
from jax.experimental.pallas import tpu as pltpu
from jax.sharding import PartitionSpec as P

MESH = pl.DeviceIdType.MESH
STEPS_BEFORE_ATTENTION = 2
PIECE = 2
LANES = 128
LEVELS = 32767.0


def kernel(
    n,
    early,
    plen_hbm,
    target_hbm,
    clen_hbm,
    cache_hbm,
    steps_hbm,
    states_hbm,
    rates_hbm,
    resident_hbm,
    token_hbm,
    query_hbm,
    res_state_hbm,
    step_size_hbm,
    inner_hbm,
    gate_hbm,
    sin_hbm,
    sout_hbm,
    skip_hbm,
    merged_hbm,
    att_ref,
    next_ref,
    mamba_ref,
    plen_ref,
    target_ref,
    clen_ref,
    cache_ref,
    steps_ref,
    rates,
    resident,
    token_ref,
    query_ref,
    res_state_ref,
    step_size_ref,
    inner_ref,
    gate_ref,
    sin_ref,
    sout_ref,
    skip_ref,
    merged,
    states,
    msteps,
    arrived,
    t_up,
    t_dn,
    h_up,
    h_dn,
    r_up,
    r_dn,
    q_up,
    q_dn,
    s_up,
    s_dn,
    part_sum,
    part_ml,
    handed,
    att_all,
    load_sem,
    go_sem,
    states_sem,
    out_sem,
    cache_send,
    cache_recv,
    pair_send,
    pair_recv,
    t_send,
    t_recv,
    h_send,
    h_recv,
    r_send,
    r_recv,
    q_send,
    q_recv,
    s_send,
    s_recv,
):
    h = n // 2
    lead = 1
    me = lax.axis_index("seq")
    core = lax.axis_index("batch")
    up = lax.rem(me + 1, n)
    down = lax.rem(me + n - 1, n)
    own, block_len, kv_heads, kv_width = cache_ref.shape
    prompts = states.shape[0]
    state = states.shape[1]
    share = handed.shape[2]
    slots, heads, head_dim = query_ref.shape
    rows = block_len * kv_heads
    own_heads = heads // n
    group = heads // kv_heads
    mine = pl.ds(core * own, own)

    pairs = (
        (plen_hbm, plen_ref),
        (steps_hbm, steps_ref.at[mine]),
        (cache_hbm, cache_ref),
        (rates_hbm, rates),
        (target_hbm, target_ref),
        (clen_hbm, clen_ref),
        (resident_hbm, resident),
        (token_hbm, token_ref),
        (query_hbm, query_ref),
        (res_state_hbm, res_state_ref),
        (step_size_hbm, step_size_ref),
        (inner_hbm, inner_ref),
        (gate_hbm, gate_ref),
        (sin_hbm, sin_ref),
        (sout_hbm, sout_ref),
        (skip_hbm, skip_ref),
    )
    loads = [
        pltpu.make_async_copy(source, held, load_sem.at[i])
        for i, (source, held) in enumerate(pairs)
    ]
    barrier = pltpu.get_barrier_semaphore()
    for neighbour in (up, down):
        pl.semaphore_signal(barrier, inc=1, device_id={"seq": neighbour}, device_id_type=MESH)
    pl.semaphore_signal(barrier, inc=1, device_id={"batch": 1 - core}, device_id_type=MESH)
    for load in loads:
        load.start()

    def columns(o):
        return pl.ds(pl.multiple_of(o * share, share), share)

    def remote(src, dst, send, recv, where):
        return pltpu.make_async_remote_copy(
            src_ref=src,
            dst_ref=dst,
            send_sem=send,
            recv_sem=recv,
            device_id=where,
            device_id_type=MESH,
        )

    def to_pair(src, dst, i):
        return remote(src, dst, pair_send.at[i], pair_recv.at[i], {"batch": 1 - core})

    def hop(buf, k, send, recv, to):
        return remote(buf.at[k], buf.at[k + 1], send, recv.at[k + 1], {"seq": to})

    def arrival(buf, k, send, recv, to):
        return remote(buf.at[k], buf.at[k], send, recv.at[k], {"seq": to})

    def send_cache(k):
        to = lax.rem(me + k, n)
        remote(
            cache_ref.at[:, to], arrived.at[mine, me], cache_send, cache_recv, {"seq": to}
        ).start()

    for load in loads[:3]:
        load.wait()
    for p in range(own):
        arrived[core * own + p, me] = cache_ref[p, me]

    theirs = pl.ds((1 - lead) * own, own)
    steps_pair = to_pair(steps_ref.at[theirs], steps_ref.at[theirs], 0)
    states_pair = to_pair(states_hbm, states.at[theirs], 1)
    states_load = pltpu.make_async_copy(states_hbm, states.at[pl.ds(lead * own, own)], states_sem)

    pl.semaphore_wait(barrier, 3)

    @pl.when(core != lead)
    def _():
        steps_pair.start()
        states_pair.start()

        def both_ways(k, carry):
            pl.semaphore_wait(go_sem, 1)
            send_cache(k)
            send_cache(n - k)
            return carry

        lax.fori_loop(1, h, both_ways, 0)
        pl.semaphore_wait(go_sem, 1)
        send_cache(h)
        steps_pair.wait_send()
        states_pair.wait_send()

    usable = []
    for p in range(prompts):
        reached = me * block_len < plen_ref[p]
        usable.append(jnp.where(reached, 1.0, 0.0).astype(jnp.float32))

    def parts_of(s):
        own_steps = msteps[:, columns(lax.rem(s + n - h, n))]
        high = jnp.where(me > s, 1.0, 0.0).astype(jnp.float32)
        return high * own_steps, (1.0 - high) * own_steps

    def first_steps(buf, s):
        above, below = parts_of(s)
        buf[0, 0:prompts, :] = above
        buf[0, prompts : 2 * prompts, :] = below

    def more_steps(buf, k, s):
        above, below = parts_of(s)
        buf[k, 0:prompts, :] += above
        buf[k, prompts : 2 * prompts, :] += below

    def let_pair_send():
        pl.semaphore_signal(go_sem, inc=1, device_id={"batch": 1 - core}, device_id_type=MESH)

    def step_ring(k, carry):
        arrival(t_up, k, t_send.at[0], t_recv.at[0], up).wait_recv()
        more_steps(t_up, k, lax.rem(me + h - 1 - k, n))

        @pl.when(k < h - 1)
        def _():
            hop(t_up, k, t_send.at[0], t_recv.at[0], up).start()

        arrival(t_dn, k, t_send.at[1], t_recv.at[1], down).wait_recv()
        more_steps(t_dn, k, lax.rem(me + n - h + k, n))
        hop(t_dn, k, t_send.at[1], t_recv.at[1], down).start()
        let_pair_send()
        send_cache(k)
        send_cache(n - k)
        return carry

    def term(p, o, behind):
        return (
            usable[p]
            * jnp.exp(-rates[:, columns(o)] * behind)
            * states[p, :, columns(o)]
        )

    def coded(buf, tops, k, p, value):
        top = jnp.maximum(jnp.max(jnp.abs(value), keepdims=True), 1e-30)
        buf[k, p] = jnp.floor(value * (LEVELS / top) + 0.5).astype(jnp.int32).astype(jnp.int16)
        tops[k, p // PIECE, p % PIECE : p % PIECE + 1, :] = jnp.broadcast_to(top, (1, LANES))

    def plain(buf, tops, k, p):
        top = tops[k, p // PIECE, p % PIECE : p % PIECE + 1, 0:1]
        return buf[k, p].astype(jnp.int32).astype(jnp.float32) * (top * (1.0 / LEVELS))

    def send_sum(way, buf, tops, k, c, to):
        piece = pl.ds(c * PIECE, PIECE)
        remote(
            tops.at[k, c], tops.at[k + 1, c], q_send.at[way], q_recv.at[way, k + 1, c], {"seq": to}
        ).start()
        remote(
            buf.at[k, piece],
            buf.at[k + 1, piece],
            r_send.at[way],
            r_recv.at[way, k + 1, c],
            {"seq": to},
        ).start()

    def wait_sum(way, buf, tops, k, c, to):
        remote(
            tops.at[k, c], tops.at[k, c], q_send.at[way], q_recv.at[way, k, c], {"seq": to}
        ).wait_recv()
        piece = buf.at[k, pl.ds(c * PIECE, PIECE)]
        remote(piece, piece, r_send.at[way], r_recv.at[way, k, c], {"seq": to}).wait_recv()

    def header_up(k, o):
        arrival(h_up, k, h_send.at[0], h_recv.at[0], up).wait_recv()
        before = jnp.where(me == 0, h_up[k, prompts : 2 * prompts, :], h_up[k, 0:prompts, :])
        return before - msteps[:, columns(o)]

    def state_step(k, first):
        o_up = lax.rem(me + 2 * n - h - k, n)
        o_dn = lax.rem(me + n - h + k, n)
        behind_up = header_up(k, o_up)
        h_up[k, 0:prompts, :] = behind_up
        hop(h_up, k, h_send.at[0], h_recv.at[0], up).start()
        arrival(h_dn, k, h_send.at[1], h_recv.at[1], down).wait_recv()
        behind_dn = jnp.where(me == n - 1, 0.0, h_dn[k])
        h_dn[k] = behind_dn + msteps[:, columns(o_dn)]

        @pl.when(k < h - 1)
        def _():
            hop(h_dn, k, h_send.at[1], h_recv.at[1], down).start()

        for c in range(prompts // PIECE):
            inside = range(c * PIECE, c * PIECE + PIECE)
            up_terms = [term(p, o_up, behind_up[p : p + 1]) for p in inside]
            dn_terms = [term(p, o_dn, behind_dn[p : p + 1]) for p in inside]
            if not first:
                wait_sum(0, r_up, q_up, k, c, up)
            for p, value in zip(inside, up_terms):
                coded(r_up, q_up, k, p, value if first else plain(r_up, q_up, k, p) + value)
            send_sum(0, r_up, q_up, k, c, up)
            wait_sum(1, r_dn, q_dn, k, c, down)
            for p, value in zip(inside, dn_terms):
                coded(r_dn, q_dn, k, p, plain(r_dn, q_dn, k, p) + value)
            send_sum(1, r_dn, q_dn, k, c, down)

    @pl.when(core == lead)
    def _():
        states_load.start()
        steps_pair.wait_recv()
        for p in range(prompts):
            msteps[p : p + 1, :] = steps_ref[p] * usable[p]
        first_steps(t_up, lax.rem(me + h - 1, n))
        hop(t_up, 0, t_send.at[0], t_recv.at[0], up).start()
        first_steps(t_dn, lax.rem(me + n - h, n))
        hop(t_dn, 0, t_send.at[1], t_recv.at[1], down).start()
        lax.fori_loop(1, h, step_ring, 0)
        arrival(t_dn, h, t_send.at[1], t_recv.at[1], down).wait_recv()
        let_pair_send()
        later = t_up[h - 1, 0:prompts, :] + t_dn[h, 0:prompts, :]
        everything = (
            later + t_up[h - 1, prompts : 2 * prompts, :] + t_dn[h, prompts : 2 * prompts, :]
        )
        start = lax.rem(me + n - h, n)
        h_up[0, 0:prompts, :] = later
        h_up[0, prompts : 2 * prompts, :] = everything
        hop(h_up, 0, h_send.at[0], h_recv.at[0], up).start()
        h_dn[0] = later + msteps[:, columns(start)]
        hop(h_dn, 0, h_send.at[1], h_recv.at[1], down).start()
        send_cache(h)
        loads[3].wait()
        states_load.wait()
        states_pair.wait_recv()
        for c in range(prompts // PIECE):
            for p in range(c * PIECE, c * PIECE + PIECE):
                coded(r_dn, q_dn, 0, p, term(p, start, later[p : p + 1]))
            send_sum(1, r_dn, q_dn, 0, c, down)
        state_step(1, True)
        lax.fori_loop(2, early, lambda k, c: (state_step(k, False), c)[1], 0)

    @pl.when(core != lead)
    def _():
        loads[3].wait()

    for load in loads[4:]:
        load.wait()

    remote(
        cache_ref.at[:, pl.ds(0, n - 1)],
        arrived.at[mine, pl.ds(0, n - 1)],
        cache_send,
        cache_recv,
        {"seq": up},
    ).wait()
    cache_pair = to_pair(arrived.at[mine], arrived.at[mine], 2)
    cache_pair.start()
    cache_pair.wait()

    def slot_facts(r):
        slot = core * slots + r
        fresh, length, place = jnp.int32(0), clen_ref[r], jnp.int32(0)
        for p in range(prompts):
            hit = target_ref[p] == slot
            fresh = jnp.where(hit, 1, fresh)
            length = jnp.where(hit, plen_ref[p], length)
            place = jnp.where(hit, p, place)
        return fresh == 1, length, place

    def attend(r, carry):
        fresh, length, place = slot_facts(r)
        chosen = jnp.where(
            fresh, arrived[place].astype(jnp.float32), resident[r].astype(jnp.float32)
        )
        position = lax.broadcasted_iota(jnp.int32, chosen.shape, 0) * n + me
        chosen = jnp.where(position < length, chosen, 0.0)
        token = jnp.broadcast_to(token_ref[r].astype(jnp.float32)[None], chosen.shape)
        chosen = jnp.where(position == length, token, chosen)
        merged[r] = chosen.astype(jnp.bfloat16)
        flat = chosen.reshape(rows, kv_width).astype(jnp.bfloat16)
        score = lax.dot_general(
            query_ref[r],
            flat[:, :head_dim],
            (((1,), (1,)), ((), ())),
            preferred_element_type=jnp.float32,
        ) * (1.0 / math.sqrt(head_dim))
        column = lax.broadcasted_iota(jnp.int32, score.shape, 1)
        row = lax.broadcasted_iota(jnp.int32, score.shape, 0)
        seen = (lax.rem(column, kv_heads) == lax.div(row, group)) & (
            lax.div(column, kv_heads) * n + me <= length
        )
        score = jnp.where(seen, score, -1e30)
        top = jnp.max(score, axis=1, keepdims=True)
        weight = jnp.where(seen, jnp.exp(score - top), 0.0)
        total = jnp.sum(weight, axis=1, keepdims=True)
        summed = jnp.dot(
            weight.astype(jnp.bfloat16), flat[:, head_dim:], preferred_element_type=jnp.float32
        )
        at = pl.ds(pl.multiple_of((core * slots + r) * heads, heads), heads)
        part_sum[at, :] = summed
        lane = lax.broadcasted_iota(jnp.int32, summed.shape, 1)
        part_ml[at, :] = jnp.where(lane < head_dim // 2, top, total)
        return carry

    lax.fori_loop(0, slots, attend, 0)
    write = pltpu.make_async_copy(merged, merged_hbm, out_sem)
    write.start()
    there = pl.ds((1 - lead) * slots * heads, slots * heads)
    sum_pair = to_pair(part_sum.at[there], part_sum.at[there], 3)
    ml_pair = to_pair(part_ml.at[there], part_ml.at[there], 4)
    handed_pair = to_pair(handed, handed, 5)
    att_pair = to_pair(att_all.at[:, pl.ds((1 - lead) * slots, slots)], att_ref, 6)

    @pl.when(core != lead)
    def _():
        sum_pair.start()
        ml_pair.start()
        sum_pair.wait_send()
        ml_pair.wait_send()

    count = own_heads * 2 * slots
    half = head_dim // 2

    def own_part(o):
        at = [pl.ds(o * own_heads + g, 2 * slots, stride=heads) for g in range(own_heads)]
        return (
            jnp.concatenate([part_sum[i, :] for i in at], 0),
            jnp.concatenate([part_ml[i, :] for i in at], 0),
        )

    def joined(one, other):
        (sum_a, ml_a), (sum_b, ml_b) = one, other
        top_a, top_b = ml_a[:, 0:1], ml_b[:, 0:1]
        top = jnp.maximum(top_a, top_b)
        f_a, f_b = jnp.exp(top_a - top), jnp.exp(top_b - top)
        lane = lax.broadcasted_iota(jnp.int32, ml_a.shape, 1)
        total = ml_a * f_a + ml_b * f_b
        return sum_a * f_a + sum_b * f_b, jnp.where(lane < half, top, total)

    def read(buf, k):
        return buf[k, 0:count, :], buf[k, count : 2 * count, :]

    def put(buf, k, value):
        buf[k, 0:count, :] = value[0]
        buf[k, count : 2 * count, :] = value[1]

    def soft_step(k):
        arrival(s_up, k, s_send.at[0], s_recv.at[0], up).wait_recv()
        put(s_up, k, joined(read(s_up, k), own_part(lax.rem(me + h - 1 - k, n))))

        @pl.when(k < h - 1)
        def _():
            hop(s_up, k, s_send.at[0], s_recv.at[0], up).start()

        arrival(s_dn, k, s_send.at[1], s_recv.at[1], down).wait_recv()
        put(s_dn, k, joined(read(s_dn, k), own_part(lax.rem(me + n - h + k, n))))
        hop(s_dn, k, s_send.at[1], s_recv.at[1], down).start()

    def both(k, carry):
        state_step(k, False)
        soft_step(k - early + 1)
        return carry

    @pl.when(core == lead)
    def _():
        sum_pair.wait_recv()
        ml_pair.wait_recv()
        put(s_up, 0, own_part(lax.rem(me + h - 1, n)))
        hop(s_up, 0, s_send.at[0], s_recv.at[0], up).start()
        put(s_dn, 0, own_part(lax.rem(me + n - h, n)))
        hop(s_dn, 0, s_send.at[1], s_recv.at[1], down).start()
        lax.fori_loop(early, h, both, 0)

        behind = header_up(h, me)
        for c in range(prompts // PIECE):
            inside = range(c * PIECE, c * PIECE + PIECE)
            own_terms = [term(p, me, behind[p : p + 1]) for p in inside]
            wait_sum(0, r_up, q_up, h, c, up)
            wait_sum(1, r_dn, q_dn, h, c, down)
            for p, value in zip(inside, own_terms):
                handed[p] = plain(r_up, q_up, h, p) + plain(r_dn, q_dn, h, p) + value
        handed_pair.start()
        lax.fori_loop(h - early + 1, h, lambda k, c: (soft_step(k), c)[1], 0)
        arrival(s_dn, h, s_send.at[1], s_recv.at[1], down).wait_recv()
        sums, mls = joined(read(s_up, h - 1), read(s_dn, h))
        att = sums / mls[:, half : half + 1]
        for g in range(own_heads):
            att_all[g] = att[g * 2 * slots : (g + 1) * 2 * slots]
            att_ref[g] = att[g * 2 * slots + lead * slots : g * 2 * slots + (lead + 1) * slots]
        att_pair.start()

    @pl.when(core != lead)
    def _():
        handed_pair.wait_recv()

    rates_here = rates[:, columns(me)]
    inner = inner_ref[...].astype(jnp.float32)
    gate = gate_ref[...].astype(jnp.float32)
    gated = gate / (1.0 + jnp.exp(-gate))
    driven = step_size_ref[...] * inner
    skipped = skip_ref[...] * inner

    def upright(row):
        square = (state, state)
        same = lax.broadcasted_iota(jnp.int32, square, 0) == lax.broadcasted_iota(
            jnp.int32, square, 1
        )
        return jnp.sum(jnp.where(same, jnp.broadcast_to(row, square), 0.0), axis=1, keepdims=True)

    for r in range(slots):
        fresh, _, place = slot_facts(r)
        begin = jnp.where(fresh, handed[place], res_state_ref[r])
        following = (
            jnp.exp(-rates_here * step_size_ref[r : r + 1, :]) * begin
            + driven[r : r + 1, :] * upright(sin_ref[r : r + 1, :])
        )
        next_ref[r] = following
        readout = jnp.sum(upright(sout_ref[r : r + 1, :]) * following, axis=0, keepdims=True)
        mamba_ref[r : r + 1, :] = (readout + skipped[r : r + 1, :]) * gated[r : r + 1, :]

    def sent(buf, first, last, send, recv, to):
        part = buf.at[pl.ds(first, last - first)]
        remote(part, part, send, recv, {"seq": to}).wait_send()

    @pl.when(core == lead)
    def _():
        sent(t_up, 0, h - 1, t_send.at[0], t_recv.at[0, 0], up)
        sent(t_dn, 0, h, t_send.at[1], t_recv.at[1, 0], down)
        sent(h_up, 0, h, h_send.at[0], h_recv.at[0, 0], up)
        sent(h_dn, 0, h - 1, h_send.at[1], h_recv.at[1, 0], down)
        sent(r_up, 1, h, r_send.at[0], r_recv.at[0, 0, 0], up)
        sent(r_dn, 0, h, r_send.at[1], r_recv.at[1, 0, 0], down)
        sent(q_up, 1, h, q_send.at[0], q_recv.at[0, 0, 0], up)
        sent(q_dn, 0, h, q_send.at[1], q_recv.at[1, 0, 0], down)
        sent(s_up, 0, h - 1, s_send.at[0], s_recv.at[0, 0], up)
        sent(s_dn, 0, h, s_send.at[1], s_recv.at[1, 0], down)
        handed_pair.wait_send()
        att_pair.wait_send()

    @pl.when(core != lead)
    def _():
        att_pair.wait_recv()

    write.wait()


def local(
    n,
    prompt_cache,
    prompt_states,
    block_steps,
    prompt_lengths,
    target_slots,
    cache_lengths,
    resident_cache,
    token_cache,
    queries,
    resident_states,
    decay_rates,
    step_sizes,
    inner_input,
    inner_gate,
    state_input,
    state_readout,
    skip_gain,
):
    own, block_len, kv_heads, kv_width = prompt_cache.shape
    prompts = prompt_lengths.shape[0]
    slots, heads, head_dim = queries.shape
    state, channels = decay_rates.shape
    share = channels // n
    h = n // 2
    own_heads = heads // n
    count = own_heads * 2 * slots
    f32, bf16 = jnp.float32, jnp.bfloat16
    vmem = pl.BlockSpec(memory_space=pltpu.VMEM)
    hbm = pl.BlockSpec(memory_space=pltpu.HBM)
    dma, vm = pltpu.SemaphoreType.DMA, pltpu.VMEM
    merged, attention, next_states, mamba_output = pl.pallas_call(
        functools.partial(kernel, n, min(STEPS_BEFORE_ATTENTION, h)),
        out_shape=(
            jax.ShapeDtypeStruct((slots, block_len, kv_heads, kv_width), bf16),
            jax.ShapeDtypeStruct((own_heads, slots, head_dim), f32),
            jax.ShapeDtypeStruct((slots, state, share), f32),
            jax.ShapeDtypeStruct((slots, share), f32),
        ),
        in_specs=[hbm] * 17,
        out_specs=(hbm, vmem, vmem, vmem),
        scratch_shapes=[
            pltpu.SMEM(prompt_lengths.shape, jnp.int32),
            pltpu.SMEM(target_slots.shape, jnp.int32),
            pltpu.SMEM(cache_lengths.shape, jnp.int32),
            vm(prompt_cache.shape, bf16),
            vm((prompts, 1, channels), f32),
            vm(decay_rates.shape, f32),
            vm((slots, block_len, kv_heads, kv_width), bf16),
            vm(token_cache.shape, bf16),
            vm(queries.shape, bf16),
            vm(resident_states.shape, f32),
            vm(step_sizes.shape, f32),
            vm(inner_input.shape, bf16),
            vm(inner_gate.shape, bf16),
            vm(state_input.shape, f32),
            vm(state_readout.shape, f32),
            vm((1, share), f32),
            vm((slots, block_len, kv_heads, kv_width), bf16),
            vm((prompts, state, channels), f32),
            vm((prompts, channels), f32),
            vm((prompts, block_len, kv_heads, kv_width), bf16),
            vm((h + 1, 2 * prompts, share), f32),
            vm((h + 1, 2 * prompts, share), f32),
            vm((h + 1, 2 * prompts, share), f32),
            vm((h + 1, prompts, share), f32),
            vm((h + 1, prompts, state, share), jnp.int16),
            vm((h + 1, prompts, state, share), jnp.int16),
            vm((h + 1, prompts // PIECE, 8, LANES), f32),
            vm((h + 1, prompts // PIECE, 8, LANES), f32),
            vm((h + 1, 2 * count, head_dim), f32),
            vm((h + 1, 2 * count, head_dim), f32),
            vm((2 * slots * heads, head_dim), f32),
            vm((2 * slots * heads, head_dim), f32),
            vm((prompts, state, share), f32),
            vm((own_heads, 2 * slots, head_dim), f32),
            dma((16,)),
            pltpu.SemaphoreType.REGULAR,
            dma,
            dma,
            dma,
            dma,
            dma((7,)),
            dma((7,)),
            dma((2,)),
            dma((2, h + 1)),
            dma((2,)),
            dma((2, h + 1)),
            dma((2,)),
            dma((2, h + 1, prompts // PIECE)),
            dma((2,)),
            dma((2, h + 1, prompts // PIECE)),
            dma((2,)),
            dma((2, h + 1)),
        ],
        compiler_params=pltpu.CompilerParams(
            collective_id=0, has_side_effects=True, vmem_limit_bytes=62 * 1024 * 1024
        ),
    )(
        prompt_lengths,
        target_slots,
        cache_lengths,
        prompt_cache,
        block_steps,
        prompt_states[:, 0],
        decay_rates,
        resident_cache[:, :, 0],
        token_cache,
        queries,
        resident_states,
        step_sizes,
        inner_input,
        inner_gate,
        state_input,
        state_readout,
        skip_gain[None],
    )
    attention = attention.transpose(1, 0, 2).astype(bf16)
    return merged[:, :, None], attention, next_states, mamba_output.astype(bf16)


def solution(mesh):
    n = mesh.shape["seq"]
    rows = ("groups", "batch")
    return jax.shard_map(
        functools.partial(local, n),
        mesh=mesh,
        in_specs=(
            P(rows, "seq", None, None),
            P(rows, "seq", None, None),
            P(rows, "seq", None),
            P("groups"),
            P("groups"),
            P(rows),
            P(rows, None, "seq", None, None),
            P(rows, None, None),
            P(rows, None, None),
            P(rows, None, "seq"),
            P(),
            P(rows, "seq"),
            P(rows, "seq"),
            P(rows, "seq"),
            P(rows, None),
            P(rows, None),
            P("seq"),
        ),
        out_specs=(
            P(rows, None, "seq", None, None),
            P(rows, "seq", None),
            P(rows, None, "seq"),
            P(rows, "seq"),
        ),
        check_vma=False,
    )
```

```python
import functools
import math

import jax
import jax.numpy as jnp
from jax import lax
from jax.experimental import pallas as pl
from jax.experimental.pallas import tpu as pltpu
from jax.sharding import PartitionSpec as P

MESH = pl.DeviceIdType.MESH
STEPS_BEFORE_ATTENTION = 9
PIECE = 2
LANES = 128
LEVELS = 32767.0


def kernel(
    n,
    early,
    plen_hbm,
    target_hbm,
    clen_hbm,
    cache_hbm,
    steps_hbm,
    states_hbm,
    rates_hbm,
    resident_hbm,
    token_hbm,
    query_hbm,
    res_state_hbm,
    step_size_hbm,
    inner_hbm,
    gate_hbm,
    sin_hbm,
    sout_hbm,
    skip_hbm,
    merged_hbm,
    att_ref,
    next_ref,
    mamba_ref,
    plen_ref,
    target_ref,
    clen_ref,
    cache_ref,
    steps_ref,
    rates,
    resident,
    token_ref,
    query_ref,
    res_state_ref,
    step_size_ref,
    inner_ref,
    gate_ref,
    sin_ref,
    sout_ref,
    skip_ref,
    merged,
    states,
    msteps,
    arrived,
    c_up,
    c_dn,
    t_up,
    t_dn,
    h_up,
    h_dn,
    r_up,
    r_dn,
    q_up,
    q_dn,
    soft_out,
    facts_out,
    soft_in,
    facts_in,
    part_sum,
    part_ml,
    handed,
    load_sem,
    states_sem,
    out_sem,
    cache_send,
    cache_recv,
    c_recv,
    pair_send,
    pair_recv,
    t_send,
    t_recv,
    h_send,
    h_recv,
    r_send,
    r_recv,
    q_send,
    q_recv,
    s_send,
    s_recv,
):
    h = n // 2
    lead = 1
    me = lax.axis_index("seq")
    core = lax.axis_index("batch")
    up = lax.rem(me + 1, n)
    down = lax.rem(me + n - 1, n)
    own, block_len, kv_heads, kv_width = cache_hbm.shape
    prompts = states.shape[0]
    state = states.shape[1]
    share = handed.shape[2]
    slots, heads, head_dim = query_ref.shape
    rows = block_len * kv_heads
    own_heads = heads // n
    group = heads // kv_heads
    mine = pl.ds(core * own, own)

    pairs = (
        (plen_hbm, plen_ref),
        (steps_hbm, steps_ref.at[mine]),
        (cache_hbm, cache_ref.at[mine]),
        (rates_hbm, rates),
        (target_hbm, target_ref),
        (clen_hbm, clen_ref),
        (resident_hbm, resident),
        (token_hbm, token_ref),
        (query_hbm, query_ref),
        (res_state_hbm, res_state_ref),
        (step_size_hbm, step_size_ref),
        (inner_hbm, inner_ref),
        (gate_hbm, gate_ref),
        (sin_hbm, sin_ref),
        (sout_hbm, sout_ref),
        (skip_hbm, skip_ref),
    )
    loads = [
        pltpu.make_async_copy(source, held, load_sem.at[i])
        for i, (source, held) in enumerate(pairs)
    ]
    barrier = pltpu.get_barrier_semaphore()
    for neighbour in (up, down):
        pl.semaphore_signal(barrier, inc=1, device_id={"seq": neighbour}, device_id_type=MESH)
    pl.semaphore_signal(barrier, inc=1, device_id={"batch": 1 - core}, device_id_type=MESH)
    for load in loads:
        load.start()

    def columns(o):
        return pl.ds(pl.multiple_of(o * share, share), share)

    def remote(src, dst, send, recv, where):
        return pltpu.make_async_remote_copy(
            src_ref=src,
            dst_ref=dst,
            send_sem=send,
            recv_sem=recv,
            device_id=where,
            device_id_type=MESH,
        )

    def to_pair(src, dst, i):
        return remote(src, dst, pair_send.at[i], pair_recv.at[i], {"batch": 1 - core})

    def hop(buf, k, send, recv, to):
        return remote(buf.at[k], buf.at[k + 1], send, recv.at[k + 1], {"seq": to})

    def arrival(buf, k, send, recv, to):
        return remote(buf.at[k], buf.at[k], send, recv.at[k], {"seq": to})

    side = h + 1

    def cache_hop(way, src, k, j):
        buf = c_up if way == 0 else c_dn
        to = up if way == 0 else down
        origin = lax.rem(me + (1 - k if way == 0 else k - 1) + n, n)

        @pl.when(j == k)
        def _():
            remote(src, arrived.at[:, origin], cache_send, cache_recv, {"seq": to}).start()

        @pl.when(j > k)
        def _():
            at = k * side + j
            remote(src, buf.at[at], cache_send, c_recv.at[way, at], {"seq": to}).start()

    def cache_first(i, carry):
        j = h - i
        cache_hop(0, cache_ref.at[:, lax.rem(me + j, n)], 1, j)

        @pl.when(j < h)
        def _():
            cache_hop(1, cache_ref.at[:, lax.rem(me + n - j, n)], 1, j)

        return carry

    def cache_phase(k, carry):
        def block(i, inner):
            j = h - i
            at = (k - 1) * side + j
            remote(c_up.at[at], c_up.at[at], cache_send, c_recv.at[0, at], {"seq": up}).wait_recv()
            cache_hop(0, c_up.at[at], k, j)

            @pl.when(j < h)
            def _():
                remote(
                    c_dn.at[at], c_dn.at[at], cache_send, c_recv.at[1, at], {"seq": down}
                ).wait_recv()
                cache_hop(1, c_dn.at[at], k, j)

            return inner

        return lax.fori_loop(0, h + 1 - k, block, carry)

    for load in loads[:3]:
        load.wait()
    theirs = pl.ds((1 - lead) * own, own)
    steps_pair = to_pair(steps_ref.at[theirs], steps_ref.at[theirs], 0)
    states_pair = to_pair(states_hbm, states.at[theirs], 1)
    lead_half = pl.ds(lead * own, own)
    lead_cache = to_pair(cache_hbm, cache_ref.at[lead_half], 2)
    states_load = pltpu.make_async_copy(states_hbm, states.at[pl.ds(lead * own, own)], states_sem)

    pl.semaphore_wait(barrier, 3)

    @pl.when(core != lead)
    def _():
        steps_pair.start()
        states_pair.start()
        lead_cache.wait_recv()
        for p in range(prompts):
            arrived[p, me] = cache_ref[p, me]

        lax.fori_loop(0, h, cache_first, 0)
        lax.fori_loop(2, h + 1, cache_phase, 0)
        steps_pair.wait_send()
        states_pair.wait_send()

    usable = []
    for p in range(prompts):
        reached = me * block_len < plen_ref[p]
        usable.append(jnp.where(reached, 1.0, 0.0).astype(jnp.float32))

    def parts_of(s):
        own_steps = msteps[:, columns(lax.rem(s + n - h, n))]
        high = jnp.where(me > s, 1.0, 0.0).astype(jnp.float32)
        return high * own_steps, (1.0 - high) * own_steps

    def first_steps(buf, s):
        above, below = parts_of(s)
        buf[0, 0:prompts, :] = above
        buf[0, prompts : 2 * prompts, :] = below

    def more_steps(buf, k, s):
        above, below = parts_of(s)
        buf[k, 0:prompts, :] += above
        buf[k, prompts : 2 * prompts, :] += below

    def step_ring(k, carry):
        arrival(t_up, k, t_send.at[0], t_recv.at[0], up).wait_recv()
        more_steps(t_up, k, lax.rem(me + h - 1 - k, n))

        @pl.when(k < h - 1)
        def _():
            hop(t_up, k, t_send.at[0], t_recv.at[0], up).start()

        arrival(t_dn, k, t_send.at[1], t_recv.at[1], down).wait_recv()
        more_steps(t_dn, k, lax.rem(me + n - h + k, n))
        hop(t_dn, k, t_send.at[1], t_recv.at[1], down).start()
        return carry

    def term(p, o, behind):
        return (
            usable[p]
            * jnp.exp(-rates[:, columns(o)] * behind)
            * states[p, :, columns(o)]
        )

    def coded(buf, tops, k, p, value):
        top = jnp.maximum(jnp.max(jnp.abs(value), keepdims=True), 1e-30)
        buf[k, p] = jnp.floor(value * (LEVELS / top) + 0.5).astype(jnp.int32).astype(jnp.int16)
        tops[k, p // PIECE, p % PIECE : p % PIECE + 1, :] = jnp.broadcast_to(top, (1, LANES))

    def plain(buf, tops, k, p):
        top = tops[k, p // PIECE, p % PIECE : p % PIECE + 1, 0:1]
        return buf[k, p].astype(jnp.int32).astype(jnp.float32) * (top * (1.0 / LEVELS))

    def send_sum(way, buf, tops, k, c, to):
        piece = pl.ds(c * PIECE, PIECE)
        remote(
            tops.at[k, c], tops.at[k + 1, c], q_send.at[way], q_recv.at[way, k + 1, c], {"seq": to}
        ).start()
        remote(
            buf.at[k, piece],
            buf.at[k + 1, piece],
            r_send.at[way],
            r_recv.at[way, k + 1, c],
            {"seq": to},
        ).start()

    def wait_sum(way, buf, tops, k, c, to):
        remote(
            tops.at[k, c], tops.at[k, c], q_send.at[way], q_recv.at[way, k, c], {"seq": to}
        ).wait_recv()
        piece = buf.at[k, pl.ds(c * PIECE, PIECE)]
        remote(piece, piece, r_send.at[way], r_recv.at[way, k, c], {"seq": to}).wait_recv()

    def header_up(k, o):
        arrival(h_up, k, h_send.at[0], h_recv.at[0], up).wait_recv()
        before = jnp.where(me == 0, h_up[k, prompts : 2 * prompts, :], h_up[k, 0:prompts, :])
        return before - msteps[:, columns(o)]

    def state_step(k, first):
        o_up = lax.rem(me + 2 * n - h - k, n)
        o_dn = lax.rem(me + n - h + k, n)
        behind_up = header_up(k, o_up)
        h_up[k, 0:prompts, :] = behind_up
        hop(h_up, k, h_send.at[0], h_recv.at[0], up).start()
        arrival(h_dn, k, h_send.at[1], h_recv.at[1], down).wait_recv()
        behind_dn = jnp.where(me == n - 1, 0.0, h_dn[k])
        h_dn[k] = behind_dn + msteps[:, columns(o_dn)]

        @pl.when(k < h - 1)
        def _():
            hop(h_dn, k, h_send.at[1], h_recv.at[1], down).start()

        for c in range(prompts // PIECE):
            inside = range(c * PIECE, c * PIECE + PIECE)
            up_terms = [term(p, o_up, behind_up[p : p + 1]) for p in inside]
            dn_terms = [term(p, o_dn, behind_dn[p : p + 1]) for p in inside]
            if not first:
                wait_sum(0, r_up, q_up, k, c, up)
            for p, value in zip(inside, up_terms):
                coded(r_up, q_up, k, p, value if first else plain(r_up, q_up, k, p) + value)
            send_sum(0, r_up, q_up, k, c, up)
            wait_sum(1, r_dn, q_dn, k, c, down)
            for p, value in zip(inside, dn_terms):
                coded(r_dn, q_dn, k, p, plain(r_dn, q_dn, k, p) + value)
            send_sum(1, r_dn, q_dn, k, c, down)

    @pl.when(core == lead)
    def _():
        lead_cache.start()
        states_load.start()
        steps_pair.wait_recv()
        for p in range(prompts):
            msteps[p : p + 1, :] = steps_ref[p] * usable[p]
        first_steps(t_up, lax.rem(me + h - 1, n))
        hop(t_up, 0, t_send.at[0], t_recv.at[0], up).start()
        first_steps(t_dn, lax.rem(me + n - h, n))
        hop(t_dn, 0, t_send.at[1], t_recv.at[1], down).start()
        lax.fori_loop(1, h, step_ring, 0)
        arrival(t_dn, h, t_send.at[1], t_recv.at[1], down).wait_recv()
        later = t_up[h - 1, 0:prompts, :] + t_dn[h, 0:prompts, :]
        everything = (
            later + t_up[h - 1, prompts : 2 * prompts, :] + t_dn[h, prompts : 2 * prompts, :]
        )
        start = lax.rem(me + n - h, n)
        h_up[0, 0:prompts, :] = later
        h_up[0, prompts : 2 * prompts, :] = everything
        hop(h_up, 0, h_send.at[0], h_recv.at[0], up).start()
        h_dn[0] = later + msteps[:, columns(start)]
        hop(h_dn, 0, h_send.at[1], h_recv.at[1], down).start()
        loads[3].wait()
        states_load.wait()
        states_pair.wait_recv()
        for c in range(prompts // PIECE):
            for p in range(c * PIECE, c * PIECE + PIECE):
                coded(r_dn, q_dn, 0, p, term(p, start, later[p : p + 1]))
            send_sum(1, r_dn, q_dn, 0, c, down)
        state_step(1, True)
        lax.fori_loop(2, early, lambda k, c: (state_step(k, False), c)[1], 0)

    @pl.when(core != lead)
    def _():
        loads[3].wait()

    for load in loads[4:]:
        load.wait()

    cache_pair = to_pair(arrived, arrived, 4)

    @pl.when(core != lead)
    def _():
        some = arrived.at[:, pl.ds(0, n - 1)]
        remote(some, some, cache_send, cache_recv, {"seq": up}).wait_recv()
        cache_pair.start()
        moved = c_up.at[pl.ds(0, h * h)]
        remote(moved, moved, cache_send, cache_recv, {"seq": up}).wait_send()
        cache_pair.wait_send()

    @pl.when(core == lead)
    def _():
        lead_cache.wait_send()
        cache_pair.wait_recv()

    def slot_facts(r):
        slot = core * slots + r
        fresh, length, place = jnp.int32(0), clen_ref[r], jnp.int32(0)
        for p in range(prompts):
            hit = target_ref[p] == slot
            fresh = jnp.where(hit, 1, fresh)
            length = jnp.where(hit, plen_ref[p], length)
            place = jnp.where(hit, p, place)
        return fresh == 1, length, place

    def attend(r, carry):
        fresh, length, place = slot_facts(r)
        chosen = jnp.where(
            fresh, arrived[place].astype(jnp.float32), resident[r].astype(jnp.float32)
        )
        position = lax.broadcasted_iota(jnp.int32, chosen.shape, 0) * n + me
        chosen = jnp.where(position < length, chosen, 0.0)
        token = jnp.broadcast_to(token_ref[r].astype(jnp.float32)[None], chosen.shape)
        chosen = jnp.where(position == length, token, chosen)
        merged[r] = chosen.astype(jnp.bfloat16)
        flat = chosen.reshape(rows, kv_width).astype(jnp.bfloat16)
        score = lax.dot_general(
            query_ref[r],
            flat[:, :head_dim],
            (((1,), (1,)), ((), ())),
            preferred_element_type=jnp.float32,
        ) * (1.0 / math.sqrt(head_dim))
        column = lax.broadcasted_iota(jnp.int32, score.shape, 1)
        row = lax.broadcasted_iota(jnp.int32, score.shape, 0)
        seen = (lax.rem(column, kv_heads) == lax.div(row, group)) & (
            lax.div(column, kv_heads) * n + me <= length
        )
        score = jnp.where(seen, score, -1e30)
        top = jnp.max(score, axis=1, keepdims=True)
        weight = jnp.where(seen, jnp.exp(score - top), 0.0)
        total = jnp.sum(weight, axis=1, keepdims=True)
        summed = jnp.dot(
            weight.astype(jnp.bfloat16), flat[:, head_dim:], preferred_element_type=jnp.float32
        )
        at = pl.ds(pl.multiple_of(r * heads, heads), heads)
        most = jnp.maximum(jnp.max(jnp.abs(summed), axis=1, keepdims=True), 1e-30)
        part_sum[at, :] = jnp.floor(summed * (LEVELS / most) + 0.5)
        lane = lax.broadcasted_iota(jnp.int32, summed.shape, 1)
        part_ml[at, :] = jnp.where(
            lane < count, top, jnp.where(lane < 2 * count, total, most * (1.0 / LEVELS))
        )
        return carry

    count = own_heads * slots
    lax.fori_loop(0, slots, attend, 0)
    write = pltpu.make_async_copy(merged, merged_hbm, out_sem)
    write.start()
    handed_pair = to_pair(handed, handed, 3)

    tall = lax.broadcasted_iota(jnp.int32, (count, LANES), 0)
    wide = lax.broadcasted_iota(jnp.int32, (count, LANES), 1)

    def pack(o):
        at = [pl.ds(o * own_heads + g, slots, stride=heads) for g in range(own_heads)]
        coarse = jnp.concatenate([part_sum[i, :] for i in at], 0)
        facts = jnp.concatenate([part_ml[i, :] for i in at], 0)
        flat = jnp.sum(jnp.where(lax.rem(wide, count) == tall, facts, 0.0), axis=0, keepdims=True)
        return coarse.astype(jnp.int32).astype(jnp.int16), flat

    def send_part(k, carry):
        to = lax.rem(me + k, n)
        soft_out[to], facts_out[to] = pack(to)
        remote(soft_out.at[to], soft_in.at[me], s_send.at[0], s_recv.at[0], {"seq": to}).start()
        remote(facts_out.at[to], facts_in.at[me], s_send.at[1], s_recv.at[1], {"seq": to}).start()
        return carry

    def both_parts(k, carry):
        send_part(h - k, carry)
        return send_part(h + k, carry)

    send_part(h, 0)
    lax.fori_loop(1, h, both_parts, 0)
    soft_in[me], facts_in[me] = pack(me)

    @pl.when(core == lead)
    def _():
        lax.fori_loop(early, h, lambda k, c: (state_step(k, False), c)[1], 0)

        behind = header_up(h, me)
        for c in range(prompts // PIECE):
            inside = range(c * PIECE, c * PIECE + PIECE)
            own_terms = [term(p, me, behind[p : p + 1]) for p in inside]
            wait_sum(0, r_up, q_up, h, c, up)
            wait_sum(1, r_dn, q_dn, h, c, down)
            for p, value in zip(inside, own_terms):
                handed[p] = plain(r_up, q_up, h, p) + plain(r_dn, q_dn, h, p) + value
        handed_pair.start()

    @pl.when(core != lead)
    def _():
        handed_pair.wait_recv()

    rates_here = rates[:, columns(me)]
    inner = inner_ref[...].astype(jnp.float32)
    gate = gate_ref[...].astype(jnp.float32)
    gated = gate / (1.0 + jnp.exp(-gate))
    driven = step_size_ref[...] * inner
    skipped = skip_ref[...] * inner

    def upright(row):
        square = (state, state)
        same = lax.broadcasted_iota(jnp.int32, square, 0) == lax.broadcasted_iota(
            jnp.int32, square, 1
        )
        return jnp.sum(jnp.where(same, jnp.broadcast_to(row, square), 0.0), axis=1, keepdims=True)

    for r in range(slots):
        fresh, _, place = slot_facts(r)
        begin = jnp.where(fresh, handed[place], res_state_ref[r])
        following = (
            jnp.exp(-rates_here * step_size_ref[r : r + 1, :]) * begin
            + driven[r : r + 1, :] * upright(sin_ref[r : r + 1, :])
        )
        next_ref[r] = following
        readout = jnp.sum(upright(sout_ref[r : r + 1, :]) * following, axis=0, keepdims=True)
        mamba_ref[r : r + 1, :] = (readout + skipped[r : r + 1, :]) * gated[r : r + 1, :]

    for buf, i in ((soft_in, 0), (facts_in, 1)):
        most_of = buf.at[pl.ds(0, n - 1)]
        remote(most_of, most_of, s_send.at[i], s_recv.at[i], {"seq": up}).wait()
    facts = facts_in[:, 0, :]
    within = lax.broadcasted_iota(jnp.int32, facts.shape, 1) < count
    tops = jnp.where(within, facts, 0.0)
    totals = jnp.where(within, pltpu.roll(facts, LANES - count, 1), 0.0)
    scales = jnp.where(within, pltpu.roll(facts, LANES - 2 * count, 1), 0.0)
    factors = jnp.exp(tops - jnp.max(tops, axis=0, keepdims=True))
    whole = jnp.sum(totals * factors, axis=0, keepdims=True)
    scales = scales * factors / jnp.where(whole > 0.0, whole, 1.0)
    gathered = jnp.zeros((count, head_dim), jnp.float32)
    for j in range(n):
        row = jnp.broadcast_to(scales[j : j + 1, :], (count, LANES))
        factor = jnp.sum(jnp.where(wide == tall, row, 0.0), axis=1, keepdims=True)
        gathered = gathered + factor * soft_in[j].astype(jnp.int32).astype(jnp.float32)
    att_ref[...] = gathered

    def sent(buf, first, last, send, recv, to):
        part = buf.at[pl.ds(first, last - first)]
        remote(part, part, send, recv, {"seq": to}).wait_send()

    @pl.when(core == lead)
    def _():
        sent(t_up, 0, h - 1, t_send.at[0], t_recv.at[0, 0], up)
        sent(t_dn, 0, h, t_send.at[1], t_recv.at[1, 0], down)
        sent(h_up, 0, h, h_send.at[0], h_recv.at[0, 0], up)
        sent(h_dn, 0, h - 1, h_send.at[1], h_recv.at[1, 0], down)
        sent(r_up, 1, h, r_send.at[0], r_recv.at[0, 0, 0], up)
        sent(r_dn, 0, h, r_send.at[1], r_recv.at[1, 0, 0], down)
        sent(q_up, 1, h, q_send.at[0], q_recv.at[0, 0, 0], up)
        sent(q_dn, 0, h, q_send.at[1], q_recv.at[1, 0, 0], down)
        handed_pair.wait_send()

    write.wait()


def local(
    n,
    prompt_cache,
    prompt_states,
    block_steps,
    prompt_lengths,
    target_slots,
    cache_lengths,
    resident_cache,
    token_cache,
    queries,
    resident_states,
    decay_rates,
    step_sizes,
    inner_input,
    inner_gate,
    state_input,
    state_readout,
    skip_gain,
):
    own, block_len, kv_heads, kv_width = prompt_cache.shape
    prompts = prompt_lengths.shape[0]
    slots, heads, head_dim = queries.shape
    state, channels = decay_rates.shape
    share = channels // n
    h = n // 2
    own_heads = heads // n
    count = own_heads * slots
    f32, bf16 = jnp.float32, jnp.bfloat16
    vmem = pl.BlockSpec(memory_space=pltpu.VMEM)
    hbm = pl.BlockSpec(memory_space=pltpu.HBM)
    dma, vm = pltpu.SemaphoreType.DMA, pltpu.VMEM
    merged, attention, next_states, mamba_output = pl.pallas_call(
        functools.partial(kernel, n, min(STEPS_BEFORE_ATTENTION, h)),
        out_shape=(
            jax.ShapeDtypeStruct((slots, block_len, kv_heads, kv_width), bf16),
            jax.ShapeDtypeStruct((count, head_dim), f32),
            jax.ShapeDtypeStruct((slots, state, share), f32),
            jax.ShapeDtypeStruct((slots, share), f32),
        ),
        in_specs=[hbm] * 17,
        out_specs=(hbm, vmem, vmem, vmem),
        scratch_shapes=[
            pltpu.SMEM(prompt_lengths.shape, jnp.int32),
            pltpu.SMEM(target_slots.shape, jnp.int32),
            pltpu.SMEM(cache_lengths.shape, jnp.int32),
            vm((prompts, block_len, kv_heads, kv_width), bf16),
            vm((prompts, 1, channels), f32),
            vm(decay_rates.shape, f32),
            vm((slots, block_len, kv_heads, kv_width), bf16),
            vm(token_cache.shape, bf16),
            vm(queries.shape, bf16),
            vm(resident_states.shape, f32),
            vm(step_sizes.shape, f32),
            vm(inner_input.shape, bf16),
            vm(inner_gate.shape, bf16),
            vm(state_input.shape, f32),
            vm(state_readout.shape, f32),
            vm((1, share), f32),
            vm((slots, block_len, kv_heads, kv_width), bf16),
            vm((prompts, state, channels), f32),
            vm((prompts, channels), f32),
            vm((prompts, block_len, kv_heads, kv_width), bf16),
            vm(((h + 1) * (h + 1), prompts, kv_heads, kv_width), bf16),
            vm(((h + 1) * (h + 1), prompts, kv_heads, kv_width), bf16),
            vm((h + 1, 2 * prompts, share), f32),
            vm((h + 1, 2 * prompts, share), f32),
            vm((h + 1, 2 * prompts, share), f32),
            vm((h + 1, prompts, share), f32),
            vm((h + 1, prompts, state, share), jnp.int16),
            vm((h + 1, prompts, state, share), jnp.int16),
            vm((h + 1, prompts // PIECE, 8, LANES), f32),
            vm((h + 1, prompts // PIECE, 8, LANES), f32),
            vm((n, count, head_dim), jnp.int16),
            vm((n, 1, LANES), f32),
            vm((n, count, head_dim), jnp.int16),
            vm((n, 1, LANES), f32),
            vm((slots * heads, head_dim), f32),
            vm((slots * heads, head_dim), f32),
            vm((prompts, state, share), f32),
            dma((16,)),
            dma,
            dma,
            dma,
            dma,
            dma((2, (h + 1) * (h + 1))),
            dma((5,)),
            dma((5,)),
            dma((2,)),
            dma((2, h + 1)),
            dma((2,)),
            dma((2, h + 1)),
            dma((2,)),
            dma((2, h + 1, prompts // PIECE)),
            dma((2,)),
            dma((2, h + 1, prompts // PIECE)),
            dma((2,)),
            dma((2,)),
        ],
        compiler_params=pltpu.CompilerParams(
            collective_id=0, has_side_effects=True, vmem_limit_bytes=62 * 1024 * 1024
        ),
    )(
        prompt_lengths,
        target_slots,
        cache_lengths,
        prompt_cache,
        block_steps,
        prompt_states[:, 0],
        decay_rates,
        resident_cache[:, :, 0],
        token_cache,
        queries,
        resident_states,
        step_sizes,
        inner_input,
        inner_gate,
        state_input,
        state_readout,
        skip_gain[None],
    )
    attention = attention.reshape(own_heads, slots, head_dim).transpose(1, 0, 2).astype(bf16)
    return merged[:, :, None], attention, next_states, mamba_output.astype(bf16)


def solution(mesh):
    n = mesh.shape["seq"]
    rows = ("groups", "batch")
    return jax.shard_map(
        functools.partial(local, n),
        mesh=mesh,
        in_specs=(
            P(rows, "seq", None, None),
            P(rows, "seq", None, None),
            P(rows, "seq", None),
            P("groups"),
            P("groups"),
            P(rows),
            P(rows, None, "seq", None, None),
            P(rows, None, None),
            P(rows, None, None),
            P(rows, None, "seq"),
            P(),
            P(rows, "seq"),
            P(rows, "seq"),
            P(rows, "seq"),
            P(rows, None),
            P(rows, None),
            P("seq"),
        ),
        out_specs=(
            P(rows, None, "seq", None, None),
            P(rows, "seq", None),
            P(rows, None, "seq"),
            P(rows, "seq"),
        ),
        check_vma=False,
    )
```

```python
import functools
import math

import jax
import jax.numpy as jnp
from jax import lax
from jax.experimental import pallas as pl
from jax.experimental.pallas import tpu as pltpu
from jax.sharding import PartitionSpec as P

MESH = pl.DeviceIdType.MESH
STEPS_BEFORE_ATTENTION = 12
PIECE = 2
LANES = 128
LEVELS = 32767.0


def kernel(
    n,
    early,
    plen_hbm,
    target_hbm,
    clen_hbm,
    cache_hbm,
    steps_hbm,
    states_hbm,
    rates_hbm,
    resident_hbm,
    token_hbm,
    query_hbm,
    res_state_hbm,
    step_size_hbm,
    inner_hbm,
    gate_hbm,
    sin_hbm,
    sout_hbm,
    skip_hbm,
    merged_hbm,
    att_ref,
    next_ref,
    mamba_ref,
    plen_ref,
    target_ref,
    clen_ref,
    cache_ref,
    steps_ref,
    rates,
    resident,
    token_ref,
    query_ref,
    res_state_ref,
    step_size_ref,
    inner_ref,
    gate_ref,
    sin_ref,
    sout_ref,
    skip_ref,
    merged,
    states,
    msteps,
    arrived,
    c_up,
    c_dn,
    t_up,
    t_dn,
    h_up,
    h_dn,
    r_up,
    r_dn,
    q_up,
    q_dn,
    soft_out,
    facts_out,
    soft_in,
    facts_in,
    part_sum,
    part_ml,
    handed,
    load_sem,
    states_sem,
    out_sem,
    cache_send,
    cache_recv,
    c_recv,
    pair_send,
    pair_recv,
    t_send,
    t_recv,
    h_send,
    h_recv,
    r_send,
    r_recv,
    q_send,
    q_recv,
    s_send,
    s_recv,
):
    h = n // 2
    lead = 1
    me = lax.axis_index("seq")
    core = lax.axis_index("batch")
    up = lax.rem(me + 1, n)
    down = lax.rem(me + n - 1, n)
    own, block_len, kv_heads, kv_width = cache_hbm.shape
    prompts = states.shape[0]
    state = states.shape[1]
    share = handed.shape[2]
    slots, heads, head_dim = query_ref.shape
    rows = block_len * kv_heads
    own_heads = heads // n
    group = heads // kv_heads
    mine = pl.ds(core * own, own)

    pairs = (
        (plen_hbm, plen_ref),
        (steps_hbm, steps_ref.at[mine]),
        (cache_hbm, cache_ref.at[mine]),
        (rates_hbm, rates),
        (target_hbm, target_ref),
        (clen_hbm, clen_ref),
        (resident_hbm, resident),
        (token_hbm, token_ref),
        (query_hbm, query_ref),
        (res_state_hbm, res_state_ref),
        (step_size_hbm, step_size_ref),
        (inner_hbm, inner_ref),
        (gate_hbm, gate_ref),
        (sin_hbm, sin_ref),
        (sout_hbm, sout_ref),
        (skip_hbm, skip_ref),
    )
    loads = [
        pltpu.make_async_copy(source, held, load_sem.at[i])
        for i, (source, held) in enumerate(pairs)
    ]
    barrier = pltpu.get_barrier_semaphore()
    for neighbour in (up, down):
        pl.semaphore_signal(barrier, inc=1, device_id={"seq": neighbour}, device_id_type=MESH)
    pl.semaphore_signal(barrier, inc=1, device_id={"batch": 1 - core}, device_id_type=MESH)
    for load in loads:
        load.start()

    def columns(o):
        return pl.ds(pl.multiple_of(o * share, share), share)

    def remote(src, dst, send, recv, where):
        return pltpu.make_async_remote_copy(
            src_ref=src,
            dst_ref=dst,
            send_sem=send,
            recv_sem=recv,
            device_id=where,
            device_id_type=MESH,
        )

    def to_pair(src, dst, i):
        return remote(src, dst, pair_send.at[i], pair_recv.at[i], {"batch": 1 - core})

    def hop(buf, k, send, recv, to):
        return remote(buf.at[k], buf.at[k + 1], send, recv.at[k + 1], {"seq": to})

    def arrival(buf, k, send, recv, to):
        return remote(buf.at[k], buf.at[k], send, recv.at[k], {"seq": to})

    side = h + 1

    def cache_hop(way, src, k, j):
        buf = c_up if way == 0 else c_dn
        to = up if way == 0 else down
        origin = lax.rem(me + (1 - k if way == 0 else k - 1) + n, n)

        @pl.when(j == k)
        def _():
            remote(src, arrived.at[:, origin], cache_send, cache_recv, {"seq": to}).start()

        @pl.when(j > k)
        def _():
            at = k * side + j
            remote(src, buf.at[at], cache_send, c_recv.at[way, at], {"seq": to}).start()

    def cache_first(i, carry):
        j = h - i
        cache_hop(0, cache_ref.at[:, lax.rem(me + j, n)], 1, j)

        @pl.when(j < h)
        def _():
            cache_hop(1, cache_ref.at[:, lax.rem(me + n - j, n)], 1, j)

        return carry

    def cache_phase(k, carry):
        def block(i, inner):
            j = h - i
            at = (k - 1) * side + j
            remote(c_up.at[at], c_up.at[at], cache_send, c_recv.at[0, at], {"seq": up}).wait_recv()
            cache_hop(0, c_up.at[at], k, j)

            @pl.when(j < h)
            def _():
                remote(
                    c_dn.at[at], c_dn.at[at], cache_send, c_recv.at[1, at], {"seq": down}
                ).wait_recv()
                cache_hop(1, c_dn.at[at], k, j)

            return inner

        return lax.fori_loop(0, h + 1 - k, block, carry)

    for load in loads[:3]:
        load.wait()
    theirs = pl.ds((1 - lead) * own, own)
    steps_pair = to_pair(steps_ref.at[theirs], steps_ref.at[theirs], 0)
    states_pair = to_pair(states_hbm, states.at[theirs], 1)
    lead_half = pl.ds(lead * own, own)
    lead_cache = to_pair(cache_hbm, cache_ref.at[lead_half], 2)
    states_load = pltpu.make_async_copy(states_hbm, states.at[pl.ds(lead * own, own)], states_sem)

    pl.semaphore_wait(barrier, 3)

    @pl.when(core != lead)
    def _():
        steps_pair.start()
        states_pair.start()
        lead_cache.wait_recv()
        for p in range(prompts):
            arrived[p, me] = cache_ref[p, me]

        lax.fori_loop(0, h, cache_first, 0)
        lax.fori_loop(2, h + 1, cache_phase, 0)
        steps_pair.wait_send()
        states_pair.wait_send()

    usable = []
    for p in range(prompts):
        reached = me * block_len < plen_ref[p]
        usable.append(jnp.where(reached, 1.0, 0.0).astype(jnp.float32))

    def parts_of(s):
        own_steps = msteps[:, columns(lax.rem(s + n - h, n))]
        high = jnp.where(me > s, 1.0, 0.0).astype(jnp.float32)
        return high * own_steps, (1.0 - high) * own_steps

    def first_steps(buf, s):
        above, below = parts_of(s)
        buf[0, 0:prompts, :] = above
        buf[0, prompts : 2 * prompts, :] = below

    def more_steps(buf, k, s):
        above, below = parts_of(s)
        buf[k, 0:prompts, :] += above
        buf[k, prompts : 2 * prompts, :] += below

    def step_ring(k, carry):
        arrival(t_up, k, t_send.at[0], t_recv.at[0], up).wait_recv()
        more_steps(t_up, k, lax.rem(me + h - 1 - k, n))

        @pl.when(k < h - 1)
        def _():
            hop(t_up, k, t_send.at[0], t_recv.at[0], up).start()

        arrival(t_dn, k, t_send.at[1], t_recv.at[1], down).wait_recv()
        more_steps(t_dn, k, lax.rem(me + n - h + k, n))
        hop(t_dn, k, t_send.at[1], t_recv.at[1], down).start()
        return carry

    def term(p, o, behind):
        return (
            usable[p]
            * jnp.exp(-rates[:, columns(o)] * behind)
            * states[p, :, columns(o)]
        )

    def coded(buf, tops, k, p, value):
        top = jnp.maximum(jnp.max(jnp.abs(value), keepdims=True), 1e-30)
        buf[k, p] = jnp.floor(value * (LEVELS / top) + 0.5).astype(jnp.int32).astype(jnp.int16)
        tops[k, p // PIECE, p % PIECE : p % PIECE + 1, :] = jnp.broadcast_to(top, (1, LANES))

    def plain(buf, tops, k, p):
        top = tops[k, p // PIECE, p % PIECE : p % PIECE + 1, 0:1]
        return buf[k, p].astype(jnp.int32).astype(jnp.float32) * (top * (1.0 / LEVELS))

    def send_sum(way, buf, tops, k, c, to):
        piece = pl.ds(c * PIECE, PIECE)
        remote(
            tops.at[k, c], tops.at[k + 1, c], q_send.at[way], q_recv.at[way, k + 1, c], {"seq": to}
        ).start()
        remote(
            buf.at[k, piece],
            buf.at[k + 1, piece],
            r_send.at[way],
            r_recv.at[way, k + 1, c],
            {"seq": to},
        ).start()

    def wait_sum(way, buf, tops, k, c, to):
        remote(
            tops.at[k, c], tops.at[k, c], q_send.at[way], q_recv.at[way, k, c], {"seq": to}
        ).wait_recv()
        piece = buf.at[k, pl.ds(c * PIECE, PIECE)]
        remote(piece, piece, r_send.at[way], r_recv.at[way, k, c], {"seq": to}).wait_recv()

    def header_up(k, o):
        arrival(h_up, k, h_send.at[0], h_recv.at[0], up).wait_recv()
        before = jnp.where(me == 0, h_up[k, prompts : 2 * prompts, :], h_up[k, 0:prompts, :])
        return before - msteps[:, columns(o)]

    def state_step(k, first):
        o_up = lax.rem(me + 2 * n - h - k, n)
        o_dn = lax.rem(me + n - h + k, n)
        behind_up = header_up(k, o_up)
        h_up[k, 0:prompts, :] = behind_up
        hop(h_up, k, h_send.at[0], h_recv.at[0], up).start()
        arrival(h_dn, k, h_send.at[1], h_recv.at[1], down).wait_recv()
        behind_dn = jnp.where(me == n - 1, 0.0, h_dn[k])
        h_dn[k] = behind_dn + msteps[:, columns(o_dn)]

        @pl.when(k < h - 1)
        def _():
            hop(h_dn, k, h_send.at[1], h_recv.at[1], down).start()

        for c in range(prompts // PIECE):
            inside = range(c * PIECE, c * PIECE + PIECE)
            up_terms = [term(p, o_up, behind_up[p : p + 1]) for p in inside]
            dn_terms = [term(p, o_dn, behind_dn[p : p + 1]) for p in inside]
            if not first:
                wait_sum(0, r_up, q_up, k, c, up)
            for p, value in zip(inside, up_terms):
                coded(r_up, q_up, k, p, value if first else plain(r_up, q_up, k, p) + value)
            send_sum(0, r_up, q_up, k, c, up)
            wait_sum(1, r_dn, q_dn, k, c, down)
            for p, value in zip(inside, dn_terms):
                coded(r_dn, q_dn, k, p, plain(r_dn, q_dn, k, p) + value)
            send_sum(1, r_dn, q_dn, k, c, down)

    @pl.when(core == lead)
    def _():
        lead_cache.start()
        states_load.start()
        steps_pair.wait_recv()
        for p in range(prompts):
            msteps[p : p + 1, :] = steps_ref[p] * usable[p]
        first_steps(t_up, lax.rem(me + h - 1, n))
        hop(t_up, 0, t_send.at[0], t_recv.at[0], up).start()
        first_steps(t_dn, lax.rem(me + n - h, n))
        hop(t_dn, 0, t_send.at[1], t_recv.at[1], down).start()
        lax.fori_loop(1, h, step_ring, 0)
        arrival(t_dn, h, t_send.at[1], t_recv.at[1], down).wait_recv()
        later = t_up[h - 1, 0:prompts, :] + t_dn[h, 0:prompts, :]
        everything = (
            later + t_up[h - 1, prompts : 2 * prompts, :] + t_dn[h, prompts : 2 * prompts, :]
        )
        start = lax.rem(me + n - h, n)
        h_up[0, 0:prompts, :] = later
        h_up[0, prompts : 2 * prompts, :] = everything
        hop(h_up, 0, h_send.at[0], h_recv.at[0], up).start()
        h_dn[0] = later + msteps[:, columns(start)]
        hop(h_dn, 0, h_send.at[1], h_recv.at[1], down).start()
        loads[3].wait()
        states_load.wait()
        states_pair.wait_recv()
        for c in range(prompts // PIECE):
            for p in range(c * PIECE, c * PIECE + PIECE):
                coded(r_dn, q_dn, 0, p, term(p, start, later[p : p + 1]))
            send_sum(1, r_dn, q_dn, 0, c, down)
        state_step(1, True)
        lax.fori_loop(2, early, lambda k, c: (state_step(k, False), c)[1], 0)

    @pl.when(core != lead)
    def _():
        loads[3].wait()

    for load in loads[4:]:
        load.wait()

    cache_pair = to_pair(arrived, arrived, 4)

    @pl.when(core != lead)
    def _():
        some = arrived.at[:, pl.ds(0, n - 1)]
        remote(some, some, cache_send, cache_recv, {"seq": up}).wait_recv()
        cache_pair.start()
        moved = c_up.at[pl.ds(0, h * h)]
        remote(moved, moved, cache_send, cache_recv, {"seq": up}).wait_send()
        cache_pair.wait_send()

    @pl.when(core == lead)
    def _():
        lead_cache.wait_send()
        cache_pair.wait_recv()

    def slot_facts(r):
        slot = core * slots + r
        fresh, length, place = jnp.int32(0), clen_ref[r], jnp.int32(0)
        for p in range(prompts):
            hit = target_ref[p] == slot
            fresh = jnp.where(hit, 1, fresh)
            length = jnp.where(hit, plen_ref[p], length)
            place = jnp.where(hit, p, place)
        return fresh == 1, length, place

    def attend(r, carry):
        fresh, length, place = slot_facts(r)
        chosen = jnp.where(
            fresh, arrived[place].astype(jnp.float32), resident[r].astype(jnp.float32)
        )
        position = lax.broadcasted_iota(jnp.int32, chosen.shape, 0) * n + me
        chosen = jnp.where(position < length, chosen, 0.0)
        token = jnp.broadcast_to(token_ref[r].astype(jnp.float32)[None], chosen.shape)
        chosen = jnp.where(position == length, token, chosen)
        merged[r] = chosen.astype(jnp.bfloat16)
        flat = chosen.reshape(rows, kv_width).astype(jnp.bfloat16)
        score = lax.dot_general(
            query_ref[r],
            flat[:, :head_dim],
            (((1,), (1,)), ((), ())),
            preferred_element_type=jnp.float32,
        ) * (1.0 / math.sqrt(head_dim))
        column = lax.broadcasted_iota(jnp.int32, score.shape, 1)
        row = lax.broadcasted_iota(jnp.int32, score.shape, 0)
        seen = (lax.rem(column, kv_heads) == lax.div(row, group)) & (
            lax.div(column, kv_heads) * n + me <= length
        )
        score = jnp.where(seen, score, -1e30)
        top = jnp.max(score, axis=1, keepdims=True)
        weight = jnp.where(seen, jnp.exp(score - top), 0.0)
        total = jnp.sum(weight, axis=1, keepdims=True)
        summed = jnp.dot(
            weight.astype(jnp.bfloat16), flat[:, head_dim:], preferred_element_type=jnp.float32
        )
        at = pl.ds(pl.multiple_of(r * heads, heads), heads)
        most = jnp.maximum(jnp.max(jnp.abs(summed), axis=1, keepdims=True), 1e-30)
        part_sum[at, :] = jnp.floor(summed * (LEVELS / most) + 0.5)
        lane = lax.broadcasted_iota(jnp.int32, summed.shape, 1)
        part_ml[at, :] = jnp.where(
            lane < count, top, jnp.where(lane < 2 * count, total, most * (1.0 / LEVELS))
        )
        return carry

    count = own_heads * slots
    lax.fori_loop(0, slots, attend, 0)
    write = pltpu.make_async_copy(merged, merged_hbm, out_sem)
    write.start()
    handed_pair = to_pair(handed, handed, 3)

    tall = lax.broadcasted_iota(jnp.int32, (count, LANES), 0)
    wide = lax.broadcasted_iota(jnp.int32, (count, LANES), 1)

    def pack(o):
        at = [pl.ds(o * own_heads + g, slots, stride=heads) for g in range(own_heads)]
        coarse = jnp.concatenate([part_sum[i, :] for i in at], 0)
        facts = jnp.concatenate([part_ml[i, :] for i in at], 0)
        flat = jnp.sum(jnp.where(lax.rem(wide, count) == tall, facts, 0.0), axis=0, keepdims=True)
        return coarse.astype(jnp.int32).astype(jnp.int16), flat

    def send_part(k, carry):
        to = lax.rem(me + k, n)
        soft_out[to], facts_out[to] = pack(to)
        remote(soft_out.at[to], soft_in.at[me], s_send.at[0], s_recv.at[0], {"seq": to}).start()
        remote(facts_out.at[to], facts_in.at[me], s_send.at[1], s_recv.at[1], {"seq": to}).start()
        return carry

    def both_parts(k, carry):
        send_part(h - k, carry)
        return send_part(h + k, carry)

    send_part(h, 0)
    lax.fori_loop(1, h, both_parts, 0)
    soft_in[me], facts_in[me] = pack(me)

    @pl.when(core == lead)
    def _():
        lax.fori_loop(early, h, lambda k, c: (state_step(k, False), c)[1], 0)

        behind = header_up(h, me)
        for c in range(prompts // PIECE):
            inside = range(c * PIECE, c * PIECE + PIECE)
            own_terms = [term(p, me, behind[p : p + 1]) for p in inside]
            wait_sum(0, r_up, q_up, h, c, up)
            wait_sum(1, r_dn, q_dn, h, c, down)
            for p, value in zip(inside, own_terms):
                handed[p] = plain(r_up, q_up, h, p) + plain(r_dn, q_dn, h, p) + value
        handed_pair.start()

    @pl.when(core != lead)
    def _():
        handed_pair.wait_recv()

    rates_here = rates[:, columns(me)]
    inner = inner_ref[...].astype(jnp.float32)
    gate = gate_ref[...].astype(jnp.float32)
    gated = gate / (1.0 + jnp.exp(-gate))
    driven = step_size_ref[...] * inner
    skipped = skip_ref[...] * inner

    def upright(row):
        square = (state, state)
        same = lax.broadcasted_iota(jnp.int32, square, 0) == lax.broadcasted_iota(
            jnp.int32, square, 1
        )
        return jnp.sum(jnp.where(same, jnp.broadcast_to(row, square), 0.0), axis=1, keepdims=True)

    for r in range(slots):
        fresh, _, place = slot_facts(r)
        begin = jnp.where(fresh, handed[place], res_state_ref[r])
        following = (
            jnp.exp(-rates_here * step_size_ref[r : r + 1, :]) * begin
            + driven[r : r + 1, :] * upright(sin_ref[r : r + 1, :])
        )
        next_ref[r] = following
        readout = jnp.sum(upright(sout_ref[r : r + 1, :]) * following, axis=0, keepdims=True)
        mamba_ref[r : r + 1, :] = (readout + skipped[r : r + 1, :]) * gated[r : r + 1, :]

    for buf, i in ((soft_in, 0), (facts_in, 1)):
        most_of = buf.at[pl.ds(0, n - 1)]
        remote(most_of, most_of, s_send.at[i], s_recv.at[i], {"seq": up}).wait()
    facts = facts_in[:, 0, :]
    within = lax.broadcasted_iota(jnp.int32, facts.shape, 1) < count
    tops = jnp.where(within, facts, 0.0)
    totals = jnp.where(within, pltpu.roll(facts, LANES - count, 1), 0.0)
    scales = jnp.where(within, pltpu.roll(facts, LANES - 2 * count, 1), 0.0)
    factors = jnp.exp(tops - jnp.max(tops, axis=0, keepdims=True))
    whole = jnp.sum(totals * factors, axis=0, keepdims=True)
    scales = scales * factors / jnp.where(whole > 0.0, whole, 1.0)
    gathered = jnp.zeros((count, head_dim), jnp.float32)
    for j in range(n):
        row = jnp.broadcast_to(scales[j : j + 1, :], (count, LANES))
        factor = jnp.sum(jnp.where(wide == tall, row, 0.0), axis=1, keepdims=True)
        gathered = gathered + factor * soft_in[j].astype(jnp.int32).astype(jnp.float32)
    att_ref[...] = gathered

    def sent(buf, first, last, send, recv, to):
        part = buf.at[pl.ds(first, last - first)]
        remote(part, part, send, recv, {"seq": to}).wait_send()

    @pl.when(core == lead)
    def _():
        sent(t_up, 0, h - 1, t_send.at[0], t_recv.at[0, 0], up)
        sent(t_dn, 0, h, t_send.at[1], t_recv.at[1, 0], down)
        sent(h_up, 0, h, h_send.at[0], h_recv.at[0, 0], up)
        sent(h_dn, 0, h - 1, h_send.at[1], h_recv.at[1, 0], down)
        sent(r_up, 1, h, r_send.at[0], r_recv.at[0, 0, 0], up)
        sent(r_dn, 0, h, r_send.at[1], r_recv.at[1, 0, 0], down)
        sent(q_up, 1, h, q_send.at[0], q_recv.at[0, 0, 0], up)
        sent(q_dn, 0, h, q_send.at[1], q_recv.at[1, 0, 0], down)
        handed_pair.wait_send()

    write.wait()


def local(
    n,
    prompt_cache,
    prompt_states,
    block_steps,
    prompt_lengths,
    target_slots,
    cache_lengths,
    resident_cache,
    token_cache,
    queries,
    resident_states,
    decay_rates,
    step_sizes,
    inner_input,
    inner_gate,
    state_input,
    state_readout,
    skip_gain,
):
    own, block_len, kv_heads, kv_width = prompt_cache.shape
    prompts = prompt_lengths.shape[0]
    slots, heads, head_dim = queries.shape
    state, channels = decay_rates.shape
    share = channels // n
    h = n // 2
    own_heads = heads // n
    count = own_heads * slots
    f32, bf16 = jnp.float32, jnp.bfloat16
    vmem = pl.BlockSpec(memory_space=pltpu.VMEM)
    hbm = pl.BlockSpec(memory_space=pltpu.HBM)
    dma, vm = pltpu.SemaphoreType.DMA, pltpu.VMEM
    merged, attention, next_states, mamba_output = pl.pallas_call(
        functools.partial(kernel, n, min(STEPS_BEFORE_ATTENTION, h)),
        out_shape=(
            jax.ShapeDtypeStruct((slots, block_len, kv_heads, kv_width), bf16),
            jax.ShapeDtypeStruct((count, head_dim), f32),
            jax.ShapeDtypeStruct((slots, state, share), f32),
            jax.ShapeDtypeStruct((slots, share), f32),
        ),
        in_specs=[hbm] * 17,
        out_specs=(hbm, vmem, vmem, vmem),
        scratch_shapes=[
            pltpu.SMEM(prompt_lengths.shape, jnp.int32),
            pltpu.SMEM(target_slots.shape, jnp.int32),
            pltpu.SMEM(cache_lengths.shape, jnp.int32),
            vm((prompts, block_len, kv_heads, kv_width), bf16),
            vm((prompts, 1, channels), f32),
            vm(decay_rates.shape, f32),
            vm((slots, block_len, kv_heads, kv_width), bf16),
            vm(token_cache.shape, bf16),
            vm(queries.shape, bf16),
            vm(resident_states.shape, f32),
            vm(step_sizes.shape, f32),
            vm(inner_input.shape, bf16),
            vm(inner_gate.shape, bf16),
            vm(state_input.shape, f32),
            vm(state_readout.shape, f32),
            vm((1, share), f32),
            vm((slots, block_len, kv_heads, kv_width), bf16),
            vm((prompts, state, channels), f32),
            vm((prompts, channels), f32),
            vm((prompts, block_len, kv_heads, kv_width), bf16),
            vm(((h + 1) * (h + 1), prompts, kv_heads, kv_width), bf16),
            vm(((h + 1) * (h + 1), prompts, kv_heads, kv_width), bf16),
            vm((h + 1, 2 * prompts, share), f32),
            vm((h + 1, 2 * prompts, share), f32),
            vm((h + 1, 2 * prompts, share), f32),
            vm((h + 1, prompts, share), f32),
            vm((h + 1, prompts, state, share), jnp.int16),
            vm((h + 1, prompts, state, share), jnp.int16),
            vm((h + 1, prompts // PIECE, 8, LANES), f32),
            vm((h + 1, prompts // PIECE, 8, LANES), f32),
            vm((n, count, head_dim), jnp.int16),
            vm((n, 1, LANES), f32),
            vm((n, count, head_dim), jnp.int16),
            vm((n, 1, LANES), f32),
            vm((slots * heads, head_dim), f32),
            vm((slots * heads, head_dim), f32),
            vm((prompts, state, share), f32),
            dma((16,)),
            dma,
            dma,
            dma,
            dma,
            dma((2, (h + 1) * (h + 1))),
            dma((5,)),
            dma((5,)),
            dma((2,)),
            dma((2, h + 1)),
            dma((2,)),
            dma((2, h + 1)),
            dma((2,)),
            dma((2, h + 1, prompts // PIECE)),
            dma((2,)),
            dma((2, h + 1, prompts // PIECE)),
            dma((2,)),
            dma((2,)),
        ],
        compiler_params=pltpu.CompilerParams(
            collective_id=0, has_side_effects=True, vmem_limit_bytes=62 * 1024 * 1024
        ),
    )(
        prompt_lengths,
        target_slots,
        cache_lengths,
        prompt_cache,
        block_steps,
        prompt_states[:, 0],
        decay_rates,
        resident_cache[:, :, 0],
        token_cache,
        queries,
        resident_states,
        step_sizes,
        inner_input,
        inner_gate,
        state_input,
        state_readout,
        skip_gain[None],
    )
    attention = attention.reshape(own_heads, slots, head_dim).transpose(1, 0, 2).astype(bf16)
    return merged[:, :, None], attention, next_states, mamba_output.astype(bf16)


def solution(mesh):
    n = mesh.shape["seq"]
    rows = ("groups", "batch")
    return jax.shard_map(
        functools.partial(local, n),
        mesh=mesh,
        in_specs=(
            P(rows, "seq", None, None),
            P(rows, "seq", None, None),
            P(rows, "seq", None),
            P("groups"),
            P("groups"),
            P(rows),
            P(rows, None, "seq", None, None),
            P(rows, None, None),
            P(rows, None, None),
            P(rows, None, "seq"),
            P(),
            P(rows, "seq"),
            P(rows, "seq"),
            P(rows, "seq"),
            P(rows, None),
            P(rows, None),
            P("seq"),
        ),
        out_specs=(
            P(rows, None, "seq", None, None),
            P(rows, "seq", None),
            P(rows, None, "seq"),
            P(rows, "seq"),
        ),
        check_vma=False,
    )
```
